1024 devices in a mesh: gx: 16 (over x_hi, z), gy: 8 (over y), gz: 8 (over x_lo, core).
Axes of the slice: x: 8 (x_hi: 2, x_lo: 4; x = x_hi * 4 + x_lo), y: 8, z: 8, core: 2. Of those that a mesh axis runs over, the one named last changes fastest.
Arguments:
- displacement: float32 [3, 256, 256, 2048], P(None, 'gx', 'gy', 'gz'), may hold values from -1.5 to 1.5
- density: float32 [256, 256, 2048], P('gx', 'gy', 'gz'), may hold values from 0.03 to 1
- stiffness: float32 [24, 24], replicated, may hold values from -9 to 9.5, as said below
Outputs:
- filtered: float32 [256, 256, 2048], P('gx', 'gy', 'gz')
- compliance: float32 [], replicated
- volume: float32 [], replicated
The draws below stay inside these ranges and needn't reach their ends.
Inputs may be any that keep to these rules, and one draw needn't show every extreme that they name: `stiffness`: symmetric and positive definite, every eigenvalue at least 0.5.
All inputs are finite; a program needn't handle non-finite values.
Results may differ from the reference program's by a relative error of at most 0.00005.
Values sent between devices are 32-bit elements; how exact they have to be, the bound alone decides.
A program may use at most 32 MiB of HBM per device.

```python
import jax
import jax.numpy as jnp
from jax import lax

NX = 256
NY = 256
NZ = 2048


def draw_density(key, part):
    levels = jax.random.uniform(key, (NX, NY, NZ), jnp.float32, 0.1, 1.0)
    rising = (1.0 + 2.0 * jnp.arange(NX, dtype=jnp.float32) / max(NX - 1, 1)) / 3.0
    return levels * rising[:, None, None]


def draw_stiffness(key, part):
    factors = jax.random.truncated_normal(key, -3.0, 3.0, (24, 24), jnp.float32)
    factors = factors / jnp.sqrt(24.0)
    return jnp.dot(factors, factors.T, precision=lax.Precision.HIGHEST) + 0.5 * jnp.eye(24, dtype=jnp.float32)


def level_of(own_key, dims, cuts, least, top_value):
    def one(axis_at, shards_of):
        steps = jax.random.uniform(jax.random.fold_in(jax.random.fold_in(own_key, 6), axis_at), (shards_of,), jnp.float32, least / len(cuts), top_value / len(cuts))
        return jnp.repeat(jnp.exp(steps), dims[axis_at] // shards_of).reshape((-1,) + (1,) * (len(dims) - axis_at - 1))

    level = one(*cuts[0])
    for cut in cuts[1:]:
        level = level * one(*cut)
    return level


def bell_draw(key, dims, deviation, bound, pieces=(), kind=jnp.bfloat16):
    values = deviation * jax.random.normal(key, dims, jnp.float32)
    if pieces:
        values = values * level_of(key, dims, pieces, -0.22, 0.18)
    return jnp.clip(values, -bound, bound).astype(kind)


def setup_inputs(seed: int = 0) -> dict:
    seeds = jax.random.split(jax.random.key(seed), 4)
    displacement = bell_draw(seeds[0], (3, NX, NY, NZ), 0.25, 1.5, ((1, 16), (2, 8), (3, 8)), jnp.float32)
    density = draw_density(jax.random.fold_in(seeds[3], 71), 0)
    stiffness = draw_stiffness(jax.random.fold_in(seeds[3], 71), 0)
    return {"displacement": displacement, "density": density, "stiffness": stiffness}


VOID_STIFFNESS = 1e-3
KERNEL = (1.0, 2.0, 3.0, 2.0, 1.0)


def smooth(values, along):
    length = values.shape[along] - 4
    summed = None
    for offset in range(5):
        section = lax.slice_in_dim(values, offset, offset + length, axis=along)
        scaled = KERNEL[offset] * section
        summed = scaled if summed is None else summed + scaled
    return summed


def side_sums(first, amount, extent):
    position = first + jnp.arange(amount, dtype=jnp.int32)
    summed = jnp.zeros((amount,), jnp.float32)
    for offset in range(5):
        inside = (position + offset - 2 >= 0) & (position + offset - 2 < extent)
        summed = summed + KERNEL[offset] * inside.astype(jnp.float32)
    return summed


def plane_energy(slab_nodes, stiffness):
    height = slab_nodes.shape[2] - 1
    length = slab_nodes.shape[3] - 1
    corner_rows = jnp.stack([slab_nodes[member, along_x, along_y:along_y + height, along_z:along_z + length].reshape(-1)
                             for member in range(3) for along_x in range(2) for along_y in range(2) for along_z in range(2)])
    product = jnp.dot(stiffness, corner_rows, precision=lax.Precision.HIGHEST, preferred_element_type=jnp.float32)
    return jnp.sum(corner_rows * product, axis=0).reshape(height, length)


def energies(node_field, stiffness, planes):
    def one_plane(plane_index):
        slab_nodes = lax.dynamic_slice_in_dim(node_field, plane_index, 2, 1)
        return plane_energy(slab_nodes, stiffness)
    return lax.map(one_plane, jnp.arange(planes, dtype=jnp.int32))


def reference(displacement, density, stiffness):
    node_field = jnp.pad(displacement, ((0, 0), (0, 1), (0, 1), (0, 1)))
    energy = energies(node_field, stiffness, NX)
    modulus = VOID_STIFFNESS + density * density * density * (1.0 - VOID_STIFFNESS)
    cell_count = float(NX * NY * NZ)
    compliance = jnp.sum(modulus * energy) / cell_count
    volume = jnp.sum(density) / cell_count
    sensitivity = -3.0 * (1.0 - VOID_STIFFNESS) * density * density * energy
    hole_sum = side_sums(0, NX, NX)[:, None, None] * side_sums(0, NY, NY)[None, :, None] * side_sums(0, NZ, NZ)[None, None, :]
    weighted = sensitivity / hole_sum
    padded = jnp.pad(weighted, 2)
    filtered = smooth(smooth(smooth(padded, 0), 1), 2)
    return filtered, compliance, volume
```

```python
import functools

import jax
import jax.numpy as jnp
from jax import lax
from jax.experimental import pallas as pl
from jax.experimental.pallas import tpu as pltpu
from jax.sharding import PartitionSpec as P

VOID = 0.001
MESH = pl.DeviceIdType.MESH
F32 = jnp.float32

S_Y, S_Z, S_YZ, S_XM, S_XY, S_XZ, S_RM, S_RY, S_RZ = range(9)
S_ZL, S_ZR, S_YD, S_YU, S_XD, S_XU, S_RF = range(9, 16)
S_XYZ, S_RYZ = 16, 17
N_SEM = 18
GO_U, GO_R = 3, 4
UNROLL_PREP, UNROLL_MAIN, UNROLL_LAST = 4, 7, 5


def rounded(v):
    return v.astype(jnp.bfloat16).astype(F32)


def taps_sum(position, extent):
    low = jnp.minimum(position, extent - 1 - position)
    return jnp.where(low == 0, F32(1 / 6), jnp.where(low == 1, F32(1 / 8), F32(1 / 9)))


def kernel(nx, ny, px, py, pz,
           disp, dens, stiff,
           out, sums,
           U, UH, G, HR, R, W, Z, F, T, L, KV, INV,
           YS, YH, HY, GY, ZS, ZX, RU, RY, RZ,
           CL, CR, CLr, CRr, YS2, YR, RF, A1, A2, A3,
           load_sem, send_sem, recv_sem, ar_send, ar_recv, go):
    gx, gy, gz = lax.axis_index("gx"), lax.axis_index("gy"), lax.axis_index("gz")
    half = px // 2
    xh, zc = gx // half, gx % half
    lane32 = lax.broadcasted_iota(jnp.int32, (32, 128), 1)
    nq = 3 * nx
    npz = 2 * pz

    def dev(x, y, z):
        return {"gx": x, "gy": y, "gz": z}

    def remote(src, dst, slot, x, y, z):
        return pltpu.make_async_remote_copy(
            src_ref=src, dst_ref=dst, send_sem=send_sem.at[slot], recv_sem=recv_sem.at[slot],
            device_id=dev(x, y, z), device_id_type=MESH)

    def when(cond, *actions):
        @pl.when(cond)
        def _():
            for act in actions:
                act()

    def wait(name, *pairs):
        with jax.named_scope(name):
            for cond, *actions in pairs:
                when(cond, *actions)

    has_yl, has_yu = gy > 0, gy < py - 1
    has_zl, has_zu = gz > 0, gz < pz - 1
    last_x, first_x, upper0, lower1 = gx == px - 1, gx == 0, gx == half, gx == half - 1
    not_last, not_first = gx < px - 1, gx > 0
    plain_down = not_first & (gx != half)

    bar = pltpu.get_barrier_semaphore()

    def signal(x, y, z):
        pl.semaphore_signal(bar, inc=1, device_id=dev(x, y, z), device_id_type=MESH)

    def signal_go(slot, x, y, z):
        pl.semaphore_signal(go.at[slot], inc=1, device_id=dev(x, y, z), device_id_type=MESH)

    def as_int(c):
        return c.astype(jnp.int32)

    key_x = xh * pz + gz
    hy = py // 2
    key_y = jnp.where(gy < hy, gy, py - 1 + hy - gy)
    key_z = zc

    def of_x(k):
        return (k // pz) * half + zc, gy, k % pz

    def of_y(k):
        return gx, jnp.where(k < hy, k, py - 1 + hy - k), gz

    def of_z(k):
        return xh * half + k, gy, gz

    groups = ((key_x, npz, of_x), (key_y, py, of_y), (key_z, half, of_z))

    when(has_zu, lambda: signal(gx, gy, gz + 1))
    when(has_zl, lambda: signal(gx, gy, gz - 1))
    when(has_yu, lambda: signal(gx, gy + 1, gz))
    when(has_yl, lambda: signal(gx, gy - 1, gz))
    when(has_yu & has_zu, lambda: signal(gx, gy + 1, gz + 1))
    when(upper0, lambda: signal(half - 1, gy, gz))

    def edges(x, cond):
        when(cond & has_yu, lambda: signal(x, gy + 1, gz))
        when(cond & has_zu, lambda: signal(x, gy, gz + 1))
        when(cond & has_yu & has_zu, lambda: signal(x, gy + 1, gz + 1))

    edges(gx + 1, not_last & (gx != half - 1))
    edges(half, first_x)
    for key, count, where_to in groups:
        def tell(k, c, where_to=where_to):
            signal(*where_to(k))
            return c

        lax.fori_loop(key + 1, count, tell, 0)
    n_wait = as_int(has_zu) + as_int(has_zl) + as_int(has_yu) + as_int(has_yl) + as_int(has_yl & has_zl) + as_int(lower1)
    n_wait = n_wait + key_x + key_y + key_z
    n_wait = n_wait + jnp.where(first_x, 0, as_int(has_yl) + as_int(has_zl) + as_int(has_yl & has_zl))

    loads = []
    for t in range(2):
        for m in range(3):
            loads.append(pltpu.make_async_copy(
                disp.at[m, :, :, pl.ds(128 * t, 128)], U.at[pl.ds(0, nx), m, t], load_sem.at[3 * t + m]))
    loads.append(pltpu.make_async_copy(stiff, KV, load_sem.at[8]))
    for t in range(2):
        loads.append(pltpu.make_async_copy(dens.at[:, :, pl.ds(128 * t, 128)], R.at[:, t], load_sem.at[6 + t]))
    for c in loads:
        c.start()

    with jax.named_scope("w_bar"):
        pl.semaphore_wait(bar, n_wait)
    when(lower1, lambda: signal_go(GO_R, 0, gy, gz))

    zero8 = jnp.zeros((8, 128), F32)
    zero32 = jnp.zeros((32, 128), F32)

    @pl.when(last_x)
    def _():
        for m in range(3):
            for t in range(2):
                U[nx, m, t] = zero32
        for t in range(2):
            YH[t, nq:nq + 8, :] = zero8
            F[nx + 2, t] = zero32
            F[nx + 3, t] = zero32
        ZX[1] = jnp.zeros((40, 128), F32)

    @pl.when(first_x)
    def _():
        for t in range(2):
            F[0, t] = zero32
            F[1, t] = zero32

    @pl.when(gy == py - 1)
    def _():
        for t in range(2):
            YH[t] = jnp.zeros((nq + 8, 128), F32)
            YR[1, t] = jnp.zeros((2 * nx, 128), F32)

    @pl.when(gy == 0)
    def _():
        for t in range(2):
            YR[0, t] = jnp.zeros((2 * nx, 128), F32)

    @pl.when(gz == pz - 1)
    def _():
        ZX[0, 0:32, :] = zero32
        ZX[1, 0:32, :] = zero32
        CLr[...] = zero32

    @pl.when((gz == pz - 1) | (gy == py - 1))
    def _():
        ZX[0, 32:40, :] = zero8
        ZX[1, 32:40, :] = zero8

    @pl.when(gz == 0)
    def _():
        CRr[...] = zero32

    for t in range(2):
        zr = lax.broadcasted_iota(jnp.int32, (256, 128), 0)
        zl = lax.broadcasted_iota(jnp.int32, (256, 128), 1) + 128 * t
        T[:, 128 * t:128 * t + 128] = jnp.maximum(3 - jnp.abs(zr - zl), 0).astype(F32).astype(jnp.bfloat16)
        yv = lax.broadcasted_iota(jnp.int32, (32, 128), 0) + gy * ny
        zv = lane32 + 128 * t + gz * 256
        INV[t] = (F32(-3.0 * (1.0 - VOID)) * taps_sum(yv, py * ny)) * taps_sum(zv, pz * 256)
    HR[...] = jnp.zeros(HR.shape, F32)

    with jax.named_scope("w_load0"):
        for c in loads[:3]:
            c.wait()
    Uf = U.reshape((nx + 1) * 3 * 2 * 32, 128)
    with jax.named_scope("c_packz"):
        acc = zero32
        for q in range(nq):
            acc = jnp.where(lane32 == q, jnp.broadcast_to(U[q // 3, q % 3, 0, :, 0:1], (32, 128)), acc)
        ZS[...] = acc
        YS[0] = Uf[pl.ds(0, nq, stride=64), :]
    with jax.named_scope("w_load1"):
        for c in loads[3:6]:
            c.wait()
    YS[1] = Uf[pl.ds(32, nq, stride=64), :]

    y_copy = remote(YS, YH.at[:, pl.ds(0, nq), :], S_Y, gx, gy - 1, gz)
    z_copy = remote(ZS, ZX.at[0, pl.ds(0, 32), :], S_Z, gx, gy, gz - 1)
    yz_copy = remote(ZS.at[pl.ds(0, 8), :], ZX.at[0, pl.ds(32, 8), :], S_YZ, gx, gy - 1, gz - 1)
    xm_copy = remote(U.at[0], U.at[nx], S_XM, gx - 1, gy, gz)
    xm_to_relay = remote(U.at[0], RU, S_RM, 0, gy, gz)
    xm_relay = remote(RU, U.at[nx], S_XM, half - 1, gy, gz)
    xy_copy = remote(YS.at[:, pl.ds(0, 8), :], YH.at[:, pl.ds(nq, 8), :], S_XY, gx - 1, gy - 1, gz)
    xy_to_relay = remote(YS.at[:, pl.ds(0, 8), :], RY, S_RY, 0, gy - 1, gz)
    xy_relay = remote(RY, YH.at[:, pl.ds(nq, 8), :], S_XY, half - 1, gy, gz)
    xz_copy = remote(ZS, ZX.at[1, pl.ds(0, 32), :], S_XZ, gx - 1, gy, gz - 1)
    xz_to_relay = remote(ZS, RZ.at[pl.ds(0, 32), :], S_RZ, 0, gy, gz - 1)
    xz_relay = remote(RZ.at[pl.ds(0, 32), :], ZX.at[1, pl.ds(0, 32), :], S_XZ, half - 1, gy, gz)
    xyz_copy = remote(ZS.at[pl.ds(0, 8), :], ZX.at[1, pl.ds(32, 8), :], S_XYZ, gx - 1, gy - 1, gz - 1)
    xyz_to_relay = remote(ZS.at[pl.ds(0, 8), :], RZ.at[pl.ds(32, 8), :], S_RYZ, 0, gy - 1, gz - 1)
    xyz_relay = remote(RZ.at[pl.ds(32, 8), :], ZX.at[1, pl.ds(32, 8), :], S_XYZ, half - 1, gy, gz)
    both_l, both_u = has_yl & has_zl, has_yu & has_zu

    when(has_zl, z_copy.start)
    when(has_yl & has_zl, yz_copy.start)
    when(has_yl, y_copy.start)
    when(plain_down, xm_copy.start)
    when(upper0, xm_to_relay.start)
    when(plain_down & has_yl, xy_copy.start)
    when(plain_down & has_zl, xz_copy.start)
    when(plain_down & both_l, xyz_copy.start)
    when(upper0 & has_yl, xy_to_relay.start)
    when(upper0 & has_zl, xz_to_relay.start)
    when(upper0 & both_l, xyz_to_relay.start)

    loads[6].wait()
    kv = KV[...]
    k_hi = rounded(kv)
    k_lo = kv - k_hi
    dr = lax.broadcasted_iota(jnp.int32, (24, 256), 0)
    cc = lax.broadcasted_iota(jnp.int32, (24, 256), 1)
    second = cc >= 112
    cl = jnp.where(second, cc - 112, cc)
    inside = cc < 224
    tau = cl >> 3
    in_main = cl < 96
    a_m = as_int(tau >= 6)
    a_ = jnp.where(in_main, a_m, (cl - 96) >> 3)
    mc_ = jnp.where(in_main, tau - 6 * a_m, cl & 7)
    ok = inside & (mc_ < 6)
    d0 = 8 * (mc_ >> 1) + 4 * a_ + (mc_ & 1)
    kb = []
    for b in range(2):
        pick = ok & (dr == d0 + 2 * b)
        b_hi = jnp.where(pick & jnp.logical_not(second), F32(1), F32(0))
        b_lo = jnp.where(pick & second, F32(1), F32(0))
        kb.append(jnp.dot(k_hi, b_hi, preferred_element_type=F32) + jnp.dot(k_lo, b_lo, preferred_element_type=F32))
    cy = lax.broadcasted_iota(jnp.int32, (16, 256), 1)
    yy = lax.broadcasted_iota(jnp.int32, (16, 256), 0) & 7
    cy = jnp.where(cy >= 112, cy - 112, cy)
    rr = jnp.where(cy < 96, cy & 7, 8)
    m0, m1 = rr == yy, rr == yy + 1
    for d in range(0, 24, 2):
        r0, r1 = (jnp.concatenate([jnp.broadcast_to(kb[b][d + k:d + k + 1, :], (8, 256)) for k in range(2)], axis=0)
                  for b in range(2))
        L[8 * d:8 * d + 16, :] = jnp.where(m0, r0, jnp.where(m1, r1, F32(0))).astype(jnp.bfloat16)

    def store_pair(p, m, t, x0, x1):
        for j in range(4):
            x = jnp.concatenate([x0[8 * j:8 * j + 8], x1[8 * j:8 * j + 8]], axis=0)
            h = x.astype(jnp.bfloat16)
            UH[p, m, t, j] = h
            g = 2.0 * x - h.astype(F32)
            G[0, p, m, t, 8 * j:8 * j + 8, :] = g[0:8]
            G[1, p, m, t, 8 * j:8 * j + 8, :] = g[8:16]
            if j > 0:
                HR[p, t, 8 * j - 8 + 2 * m:8 * j - 7 + 2 * m, :] = x0[8 * j:8 * j + 1]
                HR[p, t, 8 * j - 7 + 2 * m:8 * j - 6 + 2 * m, :] = x1[8 * j:8 * j + 1]

    def prep(p, m, zx):
        u0, u1 = U[p, m, 0], U[p, m, 1]
        s0, s1 = pltpu.roll(u0, 127, 1), pltpu.roll(u1, 127, 1)
        store_pair(p, m, 0, u0, jnp.where(lane32 == 127, s1, s0))
        store_pair(p, m, 1, u1, jnp.where(lane32 == 127, zx, s1))

    for slot, (key, count, where_to) in enumerate(groups):
        def tell(k, c, slot=slot, where_to=where_to):
            signal_go(slot, *where_to(k))
            return c

        lax.fori_loop(0, key, tell, 0)
    when(zc > 0, lambda: signal_go(GO_U, gx - 1, gy, gz))

    wait("w_z", (has_zu, z_copy.wait_recv))
    with jax.named_scope("c_prep"):
        def prep_planes(p, carry):
            for m in range(3):
                prep(p, m, pltpu.roll(ZX[0, 0:32, :], 127 - (3 * p + m), 1))
            return carry

        lax.fori_loop(0, nx, prep_planes, 0, unroll=UNROLL_PREP)

    Gf = G.reshape(2 * (nx + 1) * 3 * 2 * 40, 128)
    HRf = HR.reshape((nx + 1) * 2 * 32, 128)

    def halo_rows(first, count, zx_row, planes):
        lanes = lax.broadcasted_iota(jnp.int32, (count, 128), 1)
        rows = lax.broadcasted_iota(jnp.int32, (count, 128), 0)
        nxt = jnp.sum(jnp.where(lanes == rows, jnp.broadcast_to(zx_row, (count, 128)), 0.0), axis=1, keepdims=True)
        u0, u1 = YH[0, first:first + count, :], YH[1, first:first + count, :]
        s0, s1 = pltpu.roll(u0, 127, 1), pltpu.roll(u1, 127, 1)
        v0 = jnp.where(lanes == 127, s1, s0)
        v1 = jnp.where(lanes == 127, jnp.broadcast_to(nxt, (count, 128)), s1)
        for c, pair in enumerate(((u0, u1), (v0, v1))):
            for t in range(2):
                HY[c, t, first:first + count, :] = pair[t]
                GY[c, t, first:first + count, :] = 2.0 * pair[t] - rounded(pair[t])
        for c in range(2):
            for t in range(2):
                n = 3 * planes
                at = ((c * (nx + 1) + first // 3) * 6 + t) * 40 + 32
                Gf[pl.ds(at, n, stride=80), :] = GY[c, t, first:first + n, :]
                for m in range(3):
                    at = ((first // 3) * 2 + t) * 32 + 24 + 2 * m + c
                    if planes == 1:
                        HRf[at:at + 1, :] = HY[c, t, first + m:first + m + 1, :]
                    else:
                        HRf[pl.ds(at, planes, stride=64), :] = HY[c, t, pl.ds(first + m, planes, stride=3), :]

    def blocks(i, js, acc):
        comp, vol = acc
        rx = taps_sum(gx * nx + i, px * nx)
        for j in js:
            r0 = 8 * j
            cols = []
            for t in range(2):
                tiles = [UH[i + a, m, t, j] for a in range(2) for m in range(3)]
                tiles.append(jnp.concatenate([HR[i, t, r0:r0 + 8, :], HR[i + 1, t, r0:r0 + 8, :]], axis=0).astype(jnp.bfloat16))
                cols.append(jnp.concatenate(tiles, axis=0))
            rhs = jnp.concatenate(cols, axis=1)
            rhs = jnp.concatenate([rhs, rhs], axis=0)
            prod = jnp.dot(L[:, 0:224], rhs, preferred_element_type=F32)
            for t in range(2):
                e = None
                for d in range(24):
                    m, a, b, c = d // 8, (d // 4) % 2, (d // 2) % 2, d % 2
                    term = prod[8 * d:8 * d + 8, 128 * t:128 * t + 128] * G[c, i + a, m, t, pl.ds(r0 + b, 8), :]
                    e = term if e is None else e + term
                rho = R[i, t, r0:r0 + 8, :]
                r2 = rho * rho
                comp = comp + (VOID + (r2 * rho) * (1.0 - VOID)) * e
                vol = vol + rho
                W[i, t, r0:r0 + 8, :] = (r2 * e) * (INV[t, r0:r0 + 8, :] * rx)
        return comp, vol

    for c in loads[7:9]:
        c.wait()
    first_part = (nx - 1) // 2
    with jax.named_scope("c_main0"):
        acc = lax.fori_loop(0, first_part, lambda i, a: blocks(i, (0, 1, 2), a), (zero8, zero8), unroll=UNROLL_MAIN)
    with jax.named_scope("c_main1"):
        acc = lax.fori_loop(first_part, nx - 1, lambda i, a: blocks(i, (0, 1, 2), a), acc, unroll=UNROLL_MAIN)
    wait("w_yz", (both_u, yz_copy.wait_recv))
    wait("w_y", (has_yu, y_copy.wait_recv))
    with jax.named_scope("c_halo"):
        halo_rows(0, nq, ZX[0, 32:33, :], nx)
    with jax.named_scope("c_main2"):
        acc = lax.fori_loop(0, nx - 1, lambda i, a: blocks(i, (3,), a), acc, unroll=UNROLL_LAST)

    def relay():
        pl.semaphore_wait(go.at[GO_R], 1)
        xm_to_relay.wait_recv()
        xm_relay.start()
        when(has_yu, xy_to_relay.wait_recv, xy_relay.start)
        when(has_zu, xz_to_relay.wait_recv, xz_relay.start)
        when(both_u, xyz_to_relay.wait_recv, xyz_relay.start)

    wait("w_xm", (not_last, xm_copy.wait_recv))
    wait("w_xe", (not_last & has_yu, xy_copy.wait_recv), (not_last & has_zu, xz_copy.wait_recv),
         (not_last & both_u, xyz_copy.wait_recv))
    with jax.named_scope("c_last"):
        for m in range(3):
            prep(nx, m, pltpu.roll(ZX[1, 0:32, :], 127 - m, 1))
        halo_rows(nq, 8, ZX[1, 32:33, :], 1)
        comp, vol = blocks(nx - 1, (0, 1, 2, 3), acc)

    def stage_send(buf, stage):
        key, count, where_to = groups[stage]
        with jax.named_scope(f"w_go{stage}"):
            when(key < count - 1, lambda: pl.semaphore_wait(go.at[stage], count - 1 - key))

        def send(k, c):
            pltpu.make_async_remote_copy(
                src_ref=buf.at[key], dst_ref=buf.at[key], send_sem=ar_send.at[stage], recv_sem=ar_recv.at[stage],
                device_id=dev(*where_to(k)), device_id_type=MESH).start()
            return c

        lax.fori_loop(0, key, send, 0)
        lax.fori_loop(key + 1, count, send, 0)

    def stage_wait(buf, stage):
        count = groups[stage][1]
        part = buf.at[pl.ds(0, count - 1)]
        with jax.named_scope(f"w_ar{stage}"):
            pltpu.make_async_copy(part, part, ar_recv.at[stage]).wait()
        total = buf[0]
        for k in range(1, count):
            total = total + buf[k]
        return total

    def stage_done(buf, stage):
        part = buf.at[pl.ds(0, groups[stage][1] - 1)]
        pltpu.make_async_copy(part, part, ar_send.at[stage]).wait()

    lane1 = lax.broadcasted_iota(jnp.int32, (1, 128), 1)
    comp_all = jnp.sum(jnp.sum(comp, axis=0, keepdims=True), axis=1, keepdims=True)
    vol_all = jnp.sum(jnp.sum(vol, axis=0, keepdims=True), axis=1, keepdims=True)
    A1[key_x] = jnp.where(lane1 == 0, jnp.broadcast_to(comp_all, (1, 128)), jnp.broadcast_to(vol_all, (1, 128)))
    stage_send(A1, 0)

    with jax.named_scope("c_packw"):
        lo, hi = zero32, zero32
        for p in range(nx):
            w0, w1 = W[p, 0], W[p, 1]
            for k in range(2):
                lo = jnp.where(lane32 == 2 * p + k, jnp.broadcast_to(w0[:, k:k + 1], (32, 128)), lo)
                hi = jnp.where(lane32 == 2 * p + k, jnp.broadcast_to(w1[:, 126 + k:127 + k], (32, 128)), hi)
        even = (lane32 & 1) == 0
        CL[...] = jnp.where(even, lo, lo + 2.0 * pltpu.roll(lo, 1, 1))
        CR[...] = jnp.where(even, hi + 2.0 * pltpu.roll(hi, 127, 1), hi)
    zl_copy = remote(CL, CLr, S_ZL, gx, gy, gz - 1)
    zr_copy = remote(CR, CRr, S_ZR, gx, gy, gz + 1)
    when(has_zl, zl_copy.start)
    when(has_zu, zr_copy.start)

    def filter_z(g, carry):
        w = jnp.concatenate([jnp.concatenate([W[4 * g + k, 0], W[4 * g + k, 1]], axis=1) for k in range(4)], axis=0)
        w_hi = w.astype(jnp.bfloat16)
        w_lo = (w - w_hi.astype(F32)).astype(jnp.bfloat16)
        z = jnp.dot(w_hi, T[...], preferred_element_type=F32) + jnp.dot(w_lo, T[...], preferred_element_type=F32)
        for k in range(4):
            for t in range(2):
                Z[4 * g + k, t, 8:40, :] = z[32 * k:32 * k + 32, 128 * t:128 * t + 128]
        return carry

    with jax.named_scope("c_fz"):
        lax.fori_loop(0, nx // 4, filter_z, 0, unroll=True)

    wait("w_relay", (first_x, relay))
    wait("w_wz", (has_zu, zl_copy.wait_recv), (has_zl, zr_copy.wait_recv))
    with jax.named_scope("c_fixz"):
        left, right = CRr[...], CLr[...]
        for p in range(nx):
            Z[p, 0, 8:40, :] += jnp.where(lane32 < 2, pltpu.roll(left, (128 - 2 * p) % 128, 1), 0.0)
            Z[p, 1, 8:40, :] += jnp.where(lane32 >= 126, pltpu.roll(right, 126 - 2 * p, 1), 0.0)

    Zf = Z.reshape(nx * 2 * 48, 128)
    for t in range(2):
        for r in range(2):
            YS2[0, t, r * nx:(r + 1) * nx, :] = Zf[pl.ds(48 * t + 8 + r, nx, stride=96), :]
            YS2[1, t, r * nx:(r + 1) * nx, :] = Zf[pl.ds(48 * t + 38 + r, nx, stride=96), :]
    yd_copy = remote(YS2.at[0], YR.at[1], S_YD, gx, gy - 1, gz)
    yu_copy = remote(YS2.at[1], YR.at[0], S_YU, gx, gy + 1, gz)
    when(has_yl, yd_copy.start)
    when(has_yu, yu_copy.start)

    total = stage_wait(A1, 0)
    A2[key_y] = total
    stage_send(A2, 1)

    wait("w_wy", (has_yu, yd_copy.wait_recv), (has_yl, yu_copy.wait_recv))
    for t in range(2):
        for r in range(2):
            Zf[pl.ds(48 * t + 6 + r, nx, stride=96), :] = YR[0, t, r * nx:(r + 1) * nx, :]
            Zf[pl.ds(48 * t + 40 + r, nx, stride=96), :] = YR[1, t, r * nx:(r + 1) * nx, :]

    def filter_y(p, carry):
        for t in range(2):
            z = [Z[p, t, 6 + d:38 + d, :] for d in range(5)]
            F[p + 2, t] = 3.0 * z[2] + 2.0 * (z[1] + z[3]) + (z[0] + z[4])
        return carry

    with jax.named_scope("c_fy"):
        lax.fori_loop(0, nx, filter_y, 0, unroll=2)

    xd_copy = remote(F.at[pl.ds(2, 2)], F.at[pl.ds(nx + 2, 2)], S_XD, gx - 1, gy, gz)
    xd_to_relay = remote(F.at[pl.ds(2, 2)], RF, S_RF, 0, gy, gz)
    xd_relay = remote(RF, F.at[pl.ds(nx + 2, 2)], S_XD, half - 1, gy, gz)
    xu_copy = remote(F.at[pl.ds(nx, 2)], F.at[pl.ds(0, 2)], S_XU, gx + 1, gy, gz)
    when(plain_down, xd_copy.start)
    when(upper0, xd_to_relay.start)
    when(zc < half - 1, lambda: pl.semaphore_wait(go.at[GO_U], 1))
    when(not_last, xu_copy.start)

    def filter_x(p, carry):
        for t in range(2):
            f = [F[p + d, t] for d in range(5)]
            out[p, :, 128 * t:128 * t + 128] = 3.0 * f[2] + 2.0 * (f[1] + f[3]) + (f[0] + f[4])
        return carry

    wait("w_frelay", (first_x, xd_to_relay.wait_recv, xd_relay.start))
    with jax.named_scope("c_fx"):
        lax.fori_loop(2, nx - 2, filter_x, 0, unroll=2)
    total = stage_wait(A2, 1)
    A3[key_z] = total
    stage_send(A3, 2)

    wait("w_fd", (not_last, xd_copy.wait_recv))
    for p in (nx - 2, nx - 1):
        filter_x(p, 0)
    wait("w_fu", (not_first, xu_copy.wait_recv))
    for p in (0, 1):
        filter_x(p, 0)

    with jax.named_scope("w_sends"):
        when(has_yl, y_copy.wait_send, yd_copy.wait_send)
        when(has_zl, z_copy.wait_send, zl_copy.wait_send)
        when(has_yl & has_zl, yz_copy.wait_send)
        when(has_zu, zr_copy.wait_send)
        when(has_yu, yu_copy.wait_send)
        when(plain_down, xm_copy.wait_send, xd_copy.wait_send)
        when(plain_down & has_yl, xy_copy.wait_send)
        when(plain_down & has_zl, xz_copy.wait_send)
        when(plain_down & both_l, xyz_copy.wait_send)
        when(upper0, xm_to_relay.wait_send, xd_to_relay.wait_send)
        when(upper0 & has_yl, xy_to_relay.wait_send)
        when(upper0 & has_zl, xz_to_relay.wait_send)
        when(upper0 & both_l, xyz_to_relay.wait_send)
        when(first_x, xm_relay.wait_send, xd_relay.wait_send)
        when(first_x & has_yu, xy_relay.wait_send)
        when(first_x & has_zu, xz_relay.wait_send)
        when(first_x & both_u, xyz_relay.wait_send)
        when(not_last, xu_copy.wait_send)
        stage_done(A1, 0)
        stage_done(A2, 1)
        stage_done(A3, 2)

    total = stage_wait(A3, 2)
    count = F32(px * nx) * F32(py * ny) * F32(pz * 256)
    sums[...] = jnp.broadcast_to(total / count, (8, 128))


def on_device(displacement, density, stiffness):
    px, py, pz = lax.axis_size("gx"), lax.axis_size("gy"), lax.axis_size("gz")
    nx, ny, nz = density.shape
    nq = 3 * nx
    vm = lambda *shape: pltpu.VMEM(shape, F32)
    out, sums = pl.pallas_call(
        functools.partial(kernel, nx, ny, px, py, pz),
        out_shape=(jax.ShapeDtypeStruct((nx, ny, nz), F32), jax.ShapeDtypeStruct((8, 128), F32)),
        in_specs=[pl.BlockSpec(memory_space=pltpu.HBM)] * 3,
        out_specs=(pl.BlockSpec(memory_space=pltpu.VMEM), pl.BlockSpec(memory_space=pltpu.VMEM)),
        scratch_shapes=[
            vm(nx + 1, 3, 2, 32, 128),
            pltpu.VMEM((nx + 1, 3, 2, 4, 16, 128), jnp.bfloat16),
            vm(2, nx + 1, 3, 2, 40, 128),
            vm(nx + 1, 2, 32, 128),
            vm(nx, 2, 32, 128),
            vm(nx, 2, 32, 128),
            vm(nx, 2, 48, 128),
            vm(nx + 4, 2, 32, 128),
            pltpu.VMEM((256, 256), jnp.bfloat16),
            pltpu.VMEM((192, 256), jnp.bfloat16),
            vm(24, 24),
            vm(2, 32, 128),
            vm(2, nq, 128),
            vm(2, nq + 8, 128),
            vm(2, 2, nq + 8, 128),
            vm(2, 2, nq + 8, 128),
            vm(32, 128),
            vm(2, 40, 128),
            vm(3, 2, 32, 128),
            vm(2, 8, 128),
            vm(40, 128),
            vm(32, 128), vm(32, 128), vm(32, 128), vm(32, 128),
            vm(2, 2, 2 * nx, 128),
            vm(2, 2, 2 * nx, 128),
            vm(2, 2, 32, 128),
            vm(2 * pz, 1, 128), vm(py, 1, 128), vm(px // 2, 1, 128),
            pltpu.SemaphoreType.DMA((9,)),
            pltpu.SemaphoreType.DMA((N_SEM,)),
            pltpu.SemaphoreType.DMA((N_SEM,)),
            pltpu.SemaphoreType.DMA((3,)),
            pltpu.SemaphoreType.DMA((3,)),
            pltpu.SemaphoreType.REGULAR((5,)),
        ],
        compiler_params=pltpu.CompilerParams(collective_id=0, has_side_effects=True, vmem_limit_bytes=56_000_000),
    )(displacement, density, stiffness)
    return out, sums[0, 0], sums[0, 1]


def solution(mesh):
    return jax.shard_map(
        on_device,
        mesh=mesh,
        in_specs=(P(None, "gx", "gy", "gz"), P("gx", "gy", "gz"), P()),
        out_specs=(P("gx", "gy", "gz"), P(), P()),
        check_vma=False,
    )
```

```python
import functools

import jax
import jax.numpy as jnp
from jax import lax
from jax.experimental import pallas as pl
from jax.experimental.pallas import tpu as pltpu
from jax.sharding import PartitionSpec as P

VOID = 0.001
MESH = pl.DeviceIdType.MESH
F32 = jnp.float32

S_Y, S_Z, S_YZ, S_XM, S_XY, S_XZ, S_RM, S_RY, S_RZ = range(9)
S_ZL, S_ZR, S_YD, S_YU, S_XD, S_XU, S_RF = range(9, 16)
S_XYZ, S_RYZ = 16, 17
N_SEM = 18
GO_U, GO_R = 3, 4
UNROLL_LAST = 15


def rounded(v):
    return v.astype(jnp.bfloat16).astype(F32)


def taps_sum(position, extent):
    low = jnp.minimum(position, extent - 1 - position)
    return jnp.where(low == 0, F32(1 / 6), jnp.where(low == 1, F32(1 / 8), F32(1 / 9)))


def kernel(nx, ny, px, py, pz,
           disp, dens, stiff,
           out, sums,
           U, UH, G, HR, R, W, Z, F, T, L, KV, INV,
           YS, YH, HY, GY, ZS, ZX, RU, RY, RZ,
           CL, CR, CLr, CRr, YS2, YR, RF, A1, A2, A3,
           load_sem, send_sem, recv_sem, ar_send, ar_recv, go):
    gx, gy, gz = lax.axis_index("gx"), lax.axis_index("gy"), lax.axis_index("gz")
    half = px // 2
    xh, zc = gx // half, gx % half
    lane32 = lax.broadcasted_iota(jnp.int32, (32, 128), 1)
    nq = 3 * nx
    npz = 2 * pz

    def dev(x, y, z):
        return {"gx": x, "gy": y, "gz": z}

    def remote(src, dst, slot, x, y, z):
        return pltpu.make_async_remote_copy(
            src_ref=src, dst_ref=dst, send_sem=send_sem.at[slot], recv_sem=recv_sem.at[slot],
            device_id=dev(x, y, z), device_id_type=MESH)

    def when(cond, *actions):
        @pl.when(cond)
        def _():
            for act in actions:
                act()

    def wait(name, *pairs):
        with jax.named_scope(name):
            for cond, *actions in pairs:
                when(cond, *actions)

    loads = []
    for t in range(2):
        for m in range(3):
            loads.append(pltpu.make_async_copy(
                disp.at[m, :, :, pl.ds(128 * t, 128)], U.at[pl.ds(0, nx), m, t], load_sem.at[3 * t + m]))
    for t in range(2):
        loads.append(pltpu.make_async_copy(dens.at[:, :, pl.ds(128 * t, 128)], R.at[:, t], load_sem.at[6 + t]))
    k_load = pltpu.make_async_copy(stiff, KV, load_sem.at[8])
    for c in loads[:6] + [k_load]:
        c.start()

    has_yl, has_yu = gy > 0, gy < py - 1
    has_zl, has_zu = gz > 0, gz < pz - 1
    last_x, first_x, upper0, lower1 = gx == px - 1, gx == 0, gx == half, gx == half - 1
    not_last, not_first = gx < px - 1, gx > 0
    plain_down = not_first & (gx != half)

    bar = pltpu.get_barrier_semaphore()

    def signal(x, y, z):
        pl.semaphore_signal(bar, inc=1, device_id=dev(x, y, z), device_id_type=MESH)

    def signal_go(slot, x, y, z):
        pl.semaphore_signal(go.at[slot], inc=1, device_id=dev(x, y, z), device_id_type=MESH)

    def as_int(c):
        return c.astype(jnp.int32)

    nxc, hx, hy = pz, pz // 2, py // 2
    at_origin = lambda c: jnp.where(c, 1, 0)
    ox = at_origin((gy == 0) & (zc == 0))
    oy = at_origin((gx == 0) & (gz == 0))

    def x_rank(x):
        return jnp.where(x < hx, x, nxc - 1 + hx - x)

    def y_rank(y):
        return jnp.where(y < hy, y, py - 1 + hy - y)

    my_x, core = xh * hx + gz // 2, gz % 2

    def members_x():
        for dx in (4, 3, 5, 2, 6, 1, 7, 0) if nxc == 8 else range(nxc):
            for dc in range(2):
                if dx or dc:
                    x, c = (my_x + dx) % nxc, (core + dc) % 2
                    yield key_of_x(x, c), ((x // hx) * half + zc, gy, 2 * (x % hx) + c)

    def members_y():
        for d in (4, 3, 5, 2, 6, 1, 7) if py == 8 else range(1, py):
            y = (gy + d) % py
            yield key_of_y(y), (gx, y, gz)

    def members_z():
        for d in range(1, half):
            z = (zc + d) % half
            yield z, (xh * half + z, gy, gz)

    def key_of_x(x, c):
        return (2 * x_rank(x) + 1 - c + npz - 2 * ox) % npz

    def key_of_y(y):
        return (y_rank(y) + py - oy) % py

    groups = ((key_of_x(my_x, core), 2 * my_x + core, npz, members_x),
              (key_of_y(gy), gy, py, members_y),
              (zc, zc, half, members_z))

    def send_go(slot):
        key, _, _, members = groups[slot]
        for other, place in members():
            when(other < key, lambda: signal_go(slot, *place))

    when(has_zu, lambda: signal(gx, gy, gz + 1))
    when(has_zl, lambda: signal(gx, gy, gz - 1))
    when(has_yu, lambda: signal(gx, gy + 1, gz))
    when(has_yl, lambda: signal(gx, gy - 1, gz))
    when(has_yu & has_zu, lambda: signal(gx, gy + 1, gz + 1))
    when(upper0, lambda: signal(half - 1, gy, gz))

    def edges(x, cond):
        when(cond & has_yu, lambda: signal(x, gy + 1, gz))
        when(cond & has_zu, lambda: signal(x, gy, gz + 1))
        when(cond & has_yu & has_zu, lambda: signal(x, gy + 1, gz + 1))

    when(first_x, lambda: signal(half, gy, gz))
    edges(gx + 1, not_last & (gx != half - 1))
    edges(half, first_x)
    def of_x(k):
        r = (k + 2 * ox) % npz
        x = x_rank(r // 2)
        return (x // hx) * half + zc, gy, 2 * (x % hx) + 1 - r % 2

    def of_y(k):
        return gx, y_rank((k + oy) % py), gz

    def of_z(k):
        return xh * half + k, gy, gz

    for (key, _, count, _), place in zip(groups, (of_x, of_y, of_z)):
        def tell(k, c, place=place):
            signal(*place(k))
            return c

        lax.fori_loop(key + 1, count, tell, 0)
    n_wait = as_int(has_zu) + as_int(has_zl) + as_int(has_yu) + as_int(has_yl) + as_int(has_yl & has_zl) + as_int(lower1 | upper0)
    n_wait = n_wait + groups[0][0] + groups[1][0] + groups[2][0]
    n_wait = n_wait + jnp.where(first_x, 0, as_int(has_yl) + as_int(has_zl) + as_int(has_yl & has_zl))

    for c in loads[6:]:
        c.start()
    with jax.named_scope("w_bar0"):
        when(lower1, lambda: pl.semaphore_wait(bar, n_wait), lambda: signal_go(GO_R, 0, gy, gz))

    zero32 = jnp.zeros((32, 128), F32)
    with jax.named_scope("w_load0"):
        for c in loads[:3]:
            c.wait()
    Uf = U.reshape((nx + 1) * 3 * 2 * 32, 128)
    with jax.named_scope("c_packz"):
        acc = zero32
        for q in range(nq):
            acc = jnp.where(lane32 == q, jnp.broadcast_to(U[q // 3, q % 3, 0, :, 0:1], (32, 128)), acc)
        ZS[...] = acc
        YS[0] = Uf[pl.ds(0, nq, stride=64), :]
    with jax.named_scope("w_load1"):
        for c in loads[3:6]:
            c.wait()
    YS[1] = Uf[pl.ds(32, nq, stride=64), :]

    with jax.named_scope("w_bar"):
        when(jnp.logical_not(lower1), lambda: pl.semaphore_wait(bar, n_wait))

    y_copy = remote(YS, YH.at[:, pl.ds(0, nq), :], S_Y, gx, gy - 1, gz)
    z_copy = remote(ZS, ZX.at[0, pl.ds(0, 32), :], S_Z, gx, gy, gz - 1)
    yz_copy = remote(ZS.at[pl.ds(0, 8), :], ZX.at[0, pl.ds(32, 8), :], S_YZ, gx, gy - 1, gz - 1)
    xm_copy = remote(U.at[0], U.at[nx], S_XM, gx - 1, gy, gz)
    xm_to_relay = remote(U.at[0], RU, S_RM, 0, gy, gz)
    xm_relay = remote(RU, U.at[nx], S_XM, half - 1, gy, gz)
    xy_copy = remote(YS.at[:, pl.ds(0, 8), :], YH.at[:, pl.ds(nq, 8), :], S_XY, gx - 1, gy - 1, gz)
    xy_to_relay = remote(YS.at[:, pl.ds(0, 8), :], RY, S_RY, 0, gy - 1, gz)
    xy_relay = remote(RY, YH.at[:, pl.ds(nq, 8), :], S_XY, half - 1, gy, gz)
    xz_copy = remote(ZS, ZX.at[1, pl.ds(0, 32), :], S_XZ, gx - 1, gy, gz - 1)
    xz_to_relay = remote(ZS, RZ.at[pl.ds(0, 32), :], S_RZ, 0, gy, gz - 1)
    xz_relay = remote(RZ.at[pl.ds(0, 32), :], ZX.at[1, pl.ds(0, 32), :], S_XZ, half - 1, gy, gz)
    xyz_copy = remote(ZS.at[pl.ds(0, 8), :], ZX.at[1, pl.ds(32, 8), :], S_XYZ, gx - 1, gy - 1, gz - 1)
    xyz_to_relay = remote(ZS.at[pl.ds(0, 8), :], RZ.at[pl.ds(32, 8), :], S_RYZ, 0, gy - 1, gz - 1)
    xyz_relay = remote(RZ.at[pl.ds(32, 8), :], ZX.at[1, pl.ds(32, 8), :], S_XYZ, half - 1, gy, gz)
    both_l, both_u = has_yl & has_zl, has_yu & has_zu

    when(has_zl, z_copy.start)
    when(has_yl & has_zl, yz_copy.start)
    when(has_yl, y_copy.start)
    when(plain_down, xm_copy.start)
    when(upper0, xm_to_relay.start)
    when(plain_down & has_yl, xy_copy.start)
    when(plain_down & has_zl, xz_copy.start)
    when(plain_down & both_l, xyz_copy.start)
    when(upper0 & has_yl, xy_to_relay.start)
    when(upper0 & has_zl, xz_to_relay.start)
    when(upper0 & both_l, xyz_to_relay.start)

    send_go(0)

    zero8 = jnp.zeros((8, 128), F32)

    @pl.when(last_x)
    def _():
        for m in range(3):
            for t in range(2):
                U[nx, m, t] = zero32
        for t in range(2):
            YH[t, nq:nq + 8, :] = zero8
            F[nx + 2, t] = zero32
            F[nx + 3, t] = zero32
        ZX[1] = jnp.zeros((40, 128), F32)

    @pl.when(first_x)
    def _():
        for t in range(2):
            F[0, t] = zero32
            F[1, t] = zero32

    @pl.when(gy == py - 1)
    def _():
        for t in range(2):
            YH[t] = jnp.zeros((nq + 8, 128), F32)
            YR[1, t] = jnp.zeros((2 * nx, 128), F32)

    @pl.when(gy == 0)
    def _():
        for t in range(2):
            YR[0, t] = jnp.zeros((2 * nx, 128), F32)

    @pl.when(gz == pz - 1)
    def _():
        ZX[0, 0:32, :] = zero32
        ZX[1, 0:32, :] = zero32
        CLr[...] = zero32

    @pl.when((gz == pz - 1) | (gy == py - 1))
    def _():
        ZX[0, 32:40, :] = zero8
        ZX[1, 32:40, :] = zero8

    @pl.when(gz == 0)
    def _():
        CRr[...] = zero32

    for t in range(2):
        yv = lax.broadcasted_iota(jnp.int32, (32, 128), 0) + gy * ny
        zv = lane32 + 128 * t + gz * 256
        INV[t] = (F32(-3.0 * (1.0 - VOID)) * taps_sum(yv, py * ny)) * taps_sum(zv, pz * 256)
    HR[...] = jnp.zeros(HR.shape, F32)

    k_load.wait()
    kv = KV[...]
    k_hi = rounded(kv)
    k_lo = kv - k_hi
    dr = lax.broadcasted_iota(jnp.int32, (24, 256), 0)
    cc = lax.broadcasted_iota(jnp.int32, (24, 256), 1)
    second = cc >= 112
    cl = jnp.where(second, cc - 112, cc)
    inside = cc < 224
    tau = cl >> 3
    in_main = cl < 96
    a_m = as_int(tau >= 6)
    a_ = jnp.where(in_main, a_m, (cl - 96) >> 3)
    mc_ = jnp.where(in_main, tau - 6 * a_m, cl & 7)
    ok = inside & (mc_ < 6)
    d0 = 8 * (mc_ >> 1) + 4 * a_ + (mc_ & 1)
    kb = []
    for b in range(2):
        pick = ok & (dr == d0 + 2 * b)
        b_hi = jnp.where(pick & jnp.logical_not(second), F32(1), F32(0))
        b_lo = jnp.where(pick & second, F32(1), F32(0))
        kb.append(jnp.dot(k_hi, b_hi, preferred_element_type=F32) + jnp.dot(k_lo, b_lo, preferred_element_type=F32))
    cy = lax.broadcasted_iota(jnp.int32, (16, 256), 1)
    yy = lax.broadcasted_iota(jnp.int32, (16, 256), 0) & 7
    cy = jnp.where(cy >= 112, cy - 112, cy)
    rr = jnp.where(cy < 96, cy & 7, 8)
    m0, m1 = rr == yy, rr == yy + 1
    for d in range(0, 24, 2):
        r0, r1 = (jnp.concatenate([jnp.broadcast_to(kb[b][d + k:d + k + 1, :], (8, 256)) for k in range(2)], axis=0)
                  for b in range(2))
        L[8 * d:8 * d + 16, :] = jnp.where(m0, r0, jnp.where(m1, r1, F32(0))).astype(jnp.bfloat16)

    def store_pair(p, m, t, x0, x1):
        for j in range(4):
            x = jnp.concatenate([x0[8 * j:8 * j + 8], x1[8 * j:8 * j + 8]], axis=0)
            h = x.astype(jnp.bfloat16)
            UH[p, m, t, j] = h
            g = 2.0 * x - h.astype(F32)
            G[0, p, m, t, 8 * j:8 * j + 8, :] = g[0:8]
            G[1, p, m, t, 8 * j:8 * j + 8, :] = g[8:16]
            if j > 0:
                HR[p, t, 8 * j - 8 + 2 * m:8 * j - 7 + 2 * m, :] = x0[8 * j:8 * j + 1]
                HR[p, t, 8 * j - 7 + 2 * m:8 * j - 6 + 2 * m, :] = x1[8 * j:8 * j + 1]

    def shifted(p, m, t, zx):
        s1 = pltpu.roll(U[p, m, 1], 127, 1)
        if t == 1:
            return jnp.where(lane32 == 127, zx, s1)
        return jnp.where(lane32 == 127, s1, pltpu.roll(U[p, m, 0], 127, 1))

    def prep(p, t, z_row=None, first=0):
        for m in range(3):
            zx = None if t == 0 else pltpu.roll(z_row, 127 - (3 * p + m - first), 1)
            store_pair(p, m, t, U[p, m, t], shifted(p, m, t, zx))

    Gf = G.reshape(2 * (nx + 1) * 3 * 2 * 40, 128)
    HRf = HR.reshape((nx + 1) * 2 * 32, 128)

    def halo_rows(first, count, zx_row, planes):
        lanes = lax.broadcasted_iota(jnp.int32, (count, 128), 1)
        rows = lax.broadcasted_iota(jnp.int32, (count, 128), 0)
        nxt = jnp.sum(jnp.where(lanes == rows, jnp.broadcast_to(zx_row, (count, 128)), 0.0), axis=1, keepdims=True)
        u0, u1 = YH[0, first:first + count, :], YH[1, first:first + count, :]
        s0, s1 = pltpu.roll(u0, 127, 1), pltpu.roll(u1, 127, 1)
        v0 = jnp.where(lanes == 127, s1, s0)
        v1 = jnp.where(lanes == 127, jnp.broadcast_to(nxt, (count, 128)), s1)
        for c, pair in enumerate(((u0, u1), (v0, v1))):
            for t in range(2):
                HY[c, t, first:first + count, :] = pair[t]
                GY[c, t, first:first + count, :] = 2.0 * pair[t] - rounded(pair[t])
        for c in range(2):
            for t in range(2):
                n = 3 * planes
                at = ((c * (nx + 1) + first // 3) * 6 + t) * 40 + 32
                Gf[pl.ds(at, n, stride=80), :] = GY[c, t, first:first + n, :]
                for m in range(3):
                    at = ((first // 3) * 2 + t) * 32 + 24 + 2 * m + c
                    if planes == 1:
                        HRf[at:at + 1, :] = HY[c, t, first + m:first + m + 1, :]
                    else:
                        HRf[pl.ds(at, planes, stride=64), :] = HY[c, t, pl.ds(first + m, planes, stride=3), :]

    def pairs(todo, acc):
        comp, vol = acc
        for pair in todo:
            cols = []
            for i, j, t in pair:
                tiles = [UH[i + a, m, t, j] for a in range(2) for m in range(3)]
                tiles.append(jnp.concatenate(
                    [HR[i, t, 8 * j:8 * j + 8, :], HR[i + 1, t, 8 * j:8 * j + 8, :]], axis=0).astype(jnp.bfloat16))
                cols.append(jnp.concatenate(tiles, axis=0))
            rhs = jnp.concatenate(cols, axis=1)
            rhs = jnp.concatenate([rhs, rhs], axis=0)
            prod = jnp.dot(L[:, 0:224], rhs, preferred_element_type=F32)
            for side, (i, j, t) in enumerate(pair):
                r0 = 8 * j
                e = None
                for d in range(24):
                    m, a, b, c = d // 8, (d // 4) % 2, (d // 2) % 2, d % 2
                    term = prod[8 * d:8 * d + 8, 128 * side:128 * side + 128] * G[c, i + a, m, t, pl.ds(r0 + b, 8), :]
                    e = term if e is None else e + term
                rho = R[i, t, r0:r0 + 8, :]
                r2 = rho * rho
                comp = comp + (VOID + (r2 * rho) * (1.0 - VOID)) * e
                vol = vol + rho
                W[i, t, r0:r0 + 8, :] = (r2 * e) * (INV[t, r0:r0 + 8, :] * taps_sum(gx * nx + i, px * nx))
        return comp, vol

    def half_region(t, z_row, acc):
        for p in range(3):
            prep(p, t, z_row)
        for i in range(0, nx - 2, 2):
            for p in (i + 3, i + 4):
                if p < nx:
                    prep(p, t, z_row)
            acc = pairs([((i, 0, t), (i, 1, t)), ((i + 1, 0, t), (i + 1, 1, t)), ((i, 2, t), (i + 1, 2, t))], acc)
        return acc

    for c in loads[6:8]:
        c.wait()
    with jax.named_scope("c_main0"):
        acc = half_region(0, None, (zero8, zero8))
    wait("w_z", (has_zu, z_copy.wait_recv))
    with jax.named_scope("c_main1"):
        acc = half_region(1, ZX[0, 0:32, :], acc)
        i = nx - 2
        acc = pairs([((i, 0, 0), (i, 1, 0)), ((i, 0, 1), (i, 1, 1)), ((i, 2, 0), (i, 2, 1))], acc)
    wait("w_yz", (both_u, yz_copy.wait_recv))
    wait("w_y", (has_yu, y_copy.wait_recv))
    with jax.named_scope("c_halo"):
        halo_rows(0, nq, ZX[0, 32:33, :], nx)
    with jax.named_scope("c_main2"):
        acc = lax.fori_loop(0, nx - 1, lambda i, a: pairs([((i, 3, 0), (i, 3, 1))], a), acc, unroll=UNROLL_LAST)

    def relay():
        pl.semaphore_wait(go.at[GO_R], 1)
        when(has_yu, xy_to_relay.wait_recv, xy_relay.start)
        when(has_zu, xz_to_relay.wait_recv, xz_relay.start)
        when(both_u, xyz_to_relay.wait_recv, xyz_relay.start)
        xm_to_relay.wait_recv()
        xm_relay.start()

    wait("w_xm", (not_last, xm_copy.wait_recv))
    wait("w_xe", (not_last & has_yu, xy_copy.wait_recv), (not_last & has_zu, xz_copy.wait_recv),
         (not_last & both_u, xyz_copy.wait_recv))
    with jax.named_scope("c_last"):
        prep(nx, 0)
        prep(nx, 1, ZX[1, 0:32, :], 3 * nx)
        halo_rows(nq, 8, ZX[1, 32:33, :], 1)
        i = nx - 1
        comp, vol = pairs([((i, j, 0), (i, j, 1)) for j in range(4)], acc)

    def stage_send(buf, stage, row):
        key, me, count, members = groups[stage]
        buf[me] = row
        with jax.named_scope(f"w_go{stage}"):
            when(key < count - 1, lambda: pl.semaphore_wait(go.at[stage], count - 1 - key))
        for _, place in members():
            pltpu.make_async_remote_copy(
                src_ref=buf.at[me], dst_ref=buf.at[me], send_sem=ar_send.at[stage], recv_sem=ar_recv.at[stage],
                device_id=dev(*place), device_id_type=MESH).start()

    def stage_wait(buf, stage):
        count = groups[stage][2]
        part = buf.at[pl.ds(0, count - 1)]
        with jax.named_scope(f"w_ar{stage}"):
            pltpu.make_async_copy(part, part, ar_recv.at[stage]).wait()
        rows = [buf[k] for k in range(count)]
        while len(rows) > 1:
            rows = [a + b for a, b in zip(rows[::2], rows[1::2])]
        return rows[0]

    def stage_done(buf, stage):
        part = buf.at[pl.ds(0, groups[stage][2] - 1)]
        pltpu.make_async_copy(part, part, ar_send.at[stage]).wait()

    lane1 = lax.broadcasted_iota(jnp.int32, (1, 128), 1)
    comp_all = jnp.sum(jnp.sum(comp, axis=0, keepdims=True), axis=1, keepdims=True)
    vol_all = jnp.sum(jnp.sum(vol, axis=0, keepdims=True), axis=1, keepdims=True)
    stage_send(A1, 0, jnp.where(lane1 == 0, jnp.broadcast_to(comp_all, (1, 128)), jnp.broadcast_to(vol_all, (1, 128))))
    send_go(1)
    send_go(2)
    when(zc > 0, lambda: signal_go(GO_U, gx - 1, gy, gz))

    for t in range(2):
        zr = lax.broadcasted_iota(jnp.int32, (256, 128), 0)
        zl = lax.broadcasted_iota(jnp.int32, (256, 128), 1) + 128 * t
        T[:, 128 * t:128 * t + 128] = jnp.maximum(3 - jnp.abs(zr - zl), 0).astype(F32).astype(jnp.bfloat16)

    with jax.named_scope("c_packw"):
        lo, hi = zero32, zero32
        for p in range(nx):
            w0, w1 = W[p, 0], W[p, 1]
            for k in range(2):
                lo = jnp.where(lane32 == 2 * p + k, jnp.broadcast_to(w0[:, k:k + 1], (32, 128)), lo)
                hi = jnp.where(lane32 == 2 * p + k, jnp.broadcast_to(w1[:, 126 + k:127 + k], (32, 128)), hi)
        even = (lane32 & 1) == 0
        CL[...] = jnp.where(even, lo, lo + 2.0 * pltpu.roll(lo, 1, 1))
        CR[...] = jnp.where(even, hi + 2.0 * pltpu.roll(hi, 127, 1), hi)
    zl_copy = remote(CL, CLr, S_ZL, gx, gy, gz - 1)
    zr_copy = remote(CR, CRr, S_ZR, gx, gy, gz + 1)
    when(has_zl, zl_copy.start)
    when(has_zu, zr_copy.start)

    def filter_z(g, carry):
        w = jnp.concatenate([jnp.concatenate([W[4 * g + k, 0], W[4 * g + k, 1]], axis=1) for k in range(4)], axis=0)
        w_hi = w.astype(jnp.bfloat16)
        w_lo = (w - w_hi.astype(F32)).astype(jnp.bfloat16)
        z = jnp.dot(w_hi, T[...], preferred_element_type=F32) + jnp.dot(w_lo, T[...], preferred_element_type=F32)
        for k in range(4):
            for t in range(2):
                Z[4 * g + k, t, 8:40, :] = z[32 * k:32 * k + 32, 128 * t:128 * t + 128]
        return carry

    with jax.named_scope("c_fz"):
        lax.fori_loop(0, nx // 4, filter_z, 0, unroll=True)

    wait("w_relay", (first_x, relay))
    wait("w_wz", (has_zu, zl_copy.wait_recv), (has_zl, zr_copy.wait_recv))
    with jax.named_scope("c_fixz"):
        left, right = CRr[...], CLr[...]
        for p in range(nx):
            Z[p, 0, 8:40, :] += jnp.where(lane32 < 2, pltpu.roll(left, (128 - 2 * p) % 128, 1), 0.0)
            Z[p, 1, 8:40, :] += jnp.where(lane32 >= 126, pltpu.roll(right, 126 - 2 * p, 1), 0.0)

    Zf = Z.reshape(nx * 2 * 48, 128)
    for t in range(2):
        for r in range(2):
            YS2[0, t, r * nx:(r + 1) * nx, :] = Zf[pl.ds(48 * t + 8 + r, nx, stride=96), :]
            YS2[1, t, r * nx:(r + 1) * nx, :] = Zf[pl.ds(48 * t + 38 + r, nx, stride=96), :]
    yd_copy = remote(YS2.at[0], YR.at[1], S_YD, gx, gy - 1, gz)
    yu_copy = remote(YS2.at[1], YR.at[0], S_YU, gx, gy + 1, gz)
    when(has_yl, yd_copy.start)
    when(has_yu, yu_copy.start)

    stage_send(A2, 1, stage_wait(A1, 0))

    wait("w_wy", (has_yu, yd_copy.wait_recv), (has_yl, yu_copy.wait_recv))
    for t in range(2):
        for r in range(2):
            Zf[pl.ds(48 * t + 6 + r, nx, stride=96), :] = YR[0, t, r * nx:(r + 1) * nx, :]
            Zf[pl.ds(48 * t + 40 + r, nx, stride=96), :] = YR[1, t, r * nx:(r + 1) * nx, :]

    def filter_y(p, carry):
        for t in range(2):
            z = [Z[p, t, 6 + d:38 + d, :] for d in range(5)]
            F[p + 2, t] = 3.0 * z[2] + 2.0 * (z[1] + z[3]) + (z[0] + z[4])
        return carry

    with jax.named_scope("c_fy"):
        lax.fori_loop(0, nx, filter_y, 0, unroll=2)

    xd_copy = remote(F.at[pl.ds(2, 2)], F.at[pl.ds(nx + 2, 2)], S_XD, gx - 1, gy, gz)
    xd_to_relay = remote(F.at[pl.ds(2, 2)], RF, S_RF, 0, gy, gz)
    xd_relay = remote(RF, F.at[pl.ds(nx + 2, 2)], S_XD, half - 1, gy, gz)
    xu_copy = remote(F.at[pl.ds(nx, 2)], F.at[pl.ds(0, 2)], S_XU, gx + 1, gy, gz)
    when(plain_down, xd_copy.start)
    when(upper0, xd_to_relay.start)
    when(zc < half - 1, lambda: pl.semaphore_wait(go.at[GO_U], 1))
    when(not_last, xu_copy.start)

    def filter_x(p, carry):
        for t in range(2):
            f = [F[p + d, t] for d in range(5)]
            out[p, :, 128 * t:128 * t + 128] = 3.0 * f[2] + 2.0 * (f[1] + f[3]) + (f[0] + f[4])
        return carry

    wait("w_frelay", (first_x, xd_to_relay.wait_recv, xd_relay.start))
    with jax.named_scope("c_fx"):
        lax.fori_loop(2, nx - 2, filter_x, 0, unroll=2)
    stage_send(A3, 2, stage_wait(A2, 1))

    wait("w_fd", (not_last, xd_copy.wait_recv))
    for p in (nx - 2, nx - 1):
        filter_x(p, 0)
    wait("w_fu", (not_first, xu_copy.wait_recv))
    for p in (0, 1):
        filter_x(p, 0)

    with jax.named_scope("w_sends"):
        when(has_yl, y_copy.wait_send, yd_copy.wait_send)
        when(has_zl, z_copy.wait_send, zl_copy.wait_send)
        when(has_yl & has_zl, yz_copy.wait_send)
        when(has_zu, zr_copy.wait_send)
        when(has_yu, yu_copy.wait_send)
        when(plain_down, xm_copy.wait_send, xd_copy.wait_send)
        when(plain_down & has_yl, xy_copy.wait_send)
        when(plain_down & has_zl, xz_copy.wait_send)
        when(plain_down & both_l, xyz_copy.wait_send)
        when(upper0, xm_to_relay.wait_send, xd_to_relay.wait_send)
        when(upper0 & has_yl, xy_to_relay.wait_send)
        when(upper0 & has_zl, xz_to_relay.wait_send)
        when(upper0 & both_l, xyz_to_relay.wait_send)
        when(first_x, xm_relay.wait_send, xd_relay.wait_send)
        when(first_x & has_yu, xy_relay.wait_send)
        when(first_x & has_zu, xz_relay.wait_send)
        when(first_x & both_u, xyz_relay.wait_send)
        when(not_last, xu_copy.wait_send)
        stage_done(A1, 0)
        stage_done(A2, 1)
        stage_done(A3, 2)

    total = stage_wait(A3, 2)
    count = F32(px * nx) * F32(py * ny) * F32(pz * 256)
    sums[...] = jnp.broadcast_to(total / count, (8, 128))


def finish(out_ref, sums_ref, filtered, comp, vol, c_ref, v_ref, sem):
    copies = [pltpu.make_async_copy(out_ref, filtered, sem.at[0])]
    copies[0].start()
    c_ref[...] = sums_ref[0:1, 0:1]
    v_ref[...] = sums_ref[0:1, 1:2]
    for k, (src, dst) in enumerate(((c_ref, comp), (v_ref, vol))):
        copies.append(pltpu.make_async_copy(src, dst, sem.at[1 + k]))
        copies[-1].start()
    for c in copies:
        c.wait()


def on_device(displacement, density, stiffness):
    px, py, pz = lax.axis_size("gx"), lax.axis_size("gy"), lax.axis_size("gz")
    nx, ny, nz = density.shape
    nq = 3 * nx
    vm = lambda *shape: pltpu.VMEM(shape, F32)
    out, sums = pl.pallas_call(
        functools.partial(kernel, nx, ny, px, py, pz),
        out_shape=(jax.ShapeDtypeStruct((nx, ny, nz), F32), jax.ShapeDtypeStruct((8, 128), F32)),
        in_specs=[pl.BlockSpec(memory_space=pltpu.HBM)] * 3,
        out_specs=(pl.BlockSpec(memory_space=pltpu.VMEM), pl.BlockSpec(memory_space=pltpu.VMEM)),
        scratch_shapes=[
            vm(nx + 1, 3, 2, 32, 128),
            pltpu.VMEM((nx + 1, 3, 2, 4, 16, 128), jnp.bfloat16),
            vm(2, nx + 1, 3, 2, 40, 128),
            vm(nx + 1, 2, 32, 128),
            vm(nx, 2, 32, 128),
            vm(nx, 2, 32, 128),
            vm(nx, 2, 48, 128),
            vm(nx + 4, 2, 32, 128),
            pltpu.VMEM((256, 256), jnp.bfloat16),
            pltpu.VMEM((192, 256), jnp.bfloat16),
            vm(24, 24),
            vm(2, 32, 128),
            vm(2, nq, 128),
            vm(2, nq + 8, 128),
            vm(2, 2, nq + 8, 128),
            vm(2, 2, nq + 8, 128),
            vm(32, 128),
            vm(2, 40, 128),
            vm(3, 2, 32, 128),
            vm(2, 8, 128),
            vm(40, 128),
            vm(32, 128), vm(32, 128), vm(32, 128), vm(32, 128),
            vm(2, 2, 2 * nx, 128),
            vm(2, 2, 2 * nx, 128),
            vm(2, 2, 32, 128),
            vm(2 * pz, 1, 128), vm(py, 1, 128), vm(px // 2, 1, 128),
            pltpu.SemaphoreType.DMA((9,)),
            pltpu.SemaphoreType.DMA((N_SEM,)),
            pltpu.SemaphoreType.DMA((N_SEM,)),
            pltpu.SemaphoreType.DMA((3,)),
            pltpu.SemaphoreType.DMA((3,)),
            pltpu.SemaphoreType.REGULAR((5,)),
        ],
        compiler_params=pltpu.CompilerParams(collective_id=0, has_side_effects=True, vmem_limit_bytes=56_000_000),
    )(displacement, density, pltpu.with_memory_space_constraint(stiffness, pltpu.HBM))
    vmem = pl.BlockSpec(memory_space=pltpu.VMEM)
    out, comp, vol = pl.pallas_call(
        finish,
        out_shape=(jax.ShapeDtypeStruct((nx, ny, nz), F32), jax.ShapeDtypeStruct((1, 1), F32), jax.ShapeDtypeStruct((1, 1), F32)),
        in_specs=[vmem, vmem],
        out_specs=(pl.BlockSpec(memory_space=pltpu.HBM),) * 3,
        scratch_shapes=[pltpu.VMEM((1, 1), F32), pltpu.VMEM((1, 1), F32), pltpu.SemaphoreType.DMA((3,))],
        compiler_params=pltpu.CompilerParams(vmem_limit_bytes=4 << 20),
    )(out, sums)
    return out, comp.reshape(()), vol.reshape(())


def solution(mesh):
    return jax.shard_map(
        on_device,
        mesh=mesh,
        in_specs=(P(None, "gx", "gy", "gz"), P("gx", "gy", "gz"), P()),
        out_specs=(P("gx", "gy", "gz"), P(), P()),
        check_vma=False,
    )
```

```python
import functools

import jax
import jax.numpy as jnp
from jax import lax
from jax.experimental import pallas as pl
from jax.experimental.pallas import tpu as pltpu
from jax.sharding import PartitionSpec as P

VOID = 0.001
MESH = pl.DeviceIdType.MESH
F32 = jnp.float32

S_Y, S_Z, S_YZ, S_XM, S_XY, S_XZ, S_RM, S_RY, S_RZ = range(9)
S_ZL, S_ZR, S_YD, S_YU, S_XD, S_XU, S_RF = range(9, 16)
S_XYZ, S_RYZ = 16, 17
N_SEM = 18
GO_U, GO_R, GO_T = 3, 4, 5
UNROLL_LAST = 15


def rounded(v):
    return v.astype(jnp.bfloat16).astype(F32)


def taps_sum(position, extent):
    low = jnp.minimum(position, extent - 1 - position)
    return jnp.where(low == 0, F32(1 / 6), jnp.where(low == 1, F32(1 / 8), F32(1 / 9)))


def kernel(nx, ny, px, py, pz,
           disp, dens, stiff,
           out, sums,
           U, UH, G, HR, R, W, Z, F, T, L, KV, INV,
           YS, YH, HY, GY, ZS, ZX, RU, RY, RZ,
           CL, CR, CLr, CRr, YS2, YR, RF, A1, A2, A3,
           load_sem, send_sem, recv_sem, ar_send, ar_recv, down_send, down_recv, up_send, up_recv, go):
    gx, gy, gz = lax.axis_index("gx"), lax.axis_index("gy"), lax.axis_index("gz")
    half = px // 2
    xh, zc = gx // half, gx % half
    lane32 = lax.broadcasted_iota(jnp.int32, (32, 128), 1)
    nq = 3 * nx
    npz = 2 * pz

    def dev(x, y, z):
        return {"gx": x, "gy": y, "gz": z}

    def remote(src, dst, slot, x, y, z):
        return pltpu.make_async_remote_copy(
            src_ref=src, dst_ref=dst, send_sem=send_sem.at[slot], recv_sem=recv_sem.at[slot],
            device_id=dev(x, y, z), device_id_type=MESH)

    def when(cond, *actions):
        @pl.when(cond)
        def _():
            for act in actions:
                act()

    def wait(name, *pairs):
        with jax.named_scope(name):
            for cond, *actions in pairs:
                when(cond, *actions)

    loads = []
    for t in range(2):
        for m in range(3):
            loads.append(pltpu.make_async_copy(
                disp.at[m, :, :, pl.ds(128 * t, 128)], U.at[pl.ds(0, nx), m, t], load_sem.at[3 * t + m]))
    for t in range(2):
        loads.append(pltpu.make_async_copy(dens.at[:, :, pl.ds(128 * t, 128)], R.at[:, t], load_sem.at[6 + t]))
    k_load = pltpu.make_async_copy(stiff, KV, load_sem.at[8])
    for c in loads[:6] + [k_load]:
        c.start()

    has_yl, has_yu = gy > 0, gy < py - 1
    has_zl, has_zu = gz > 0, gz < pz - 1
    last_x, first_x, upper0, lower1 = gx == px - 1, gx == 0, gx == half, gx == half - 1
    not_last, not_first = gx < px - 1, gx > 0
    plain_down = not_first & (gx != half)

    bar = pltpu.get_barrier_semaphore()

    def signal(x, y, z):
        pl.semaphore_signal(bar, inc=1, device_id=dev(x, y, z), device_id_type=MESH)

    def signal_go(slot, x, y, z):
        pl.semaphore_signal(go.at[slot], inc=1, device_id=dev(x, y, z), device_id_type=MESH)

    def as_int(c):
        return c.astype(jnp.int32)

    nxc, hx, hy = pz, pz // 2, py // 2
    at_origin = lambda c: jnp.where(c, 1, 0)
    ox = at_origin((gy == 0) & (zc == 0))
    oy = at_origin((gx == 0) & (gz == 0))

    def x_rank(x):
        return jnp.where(x < hx, x, nxc - 1 + hx - x)

    def y_rank(y):
        return jnp.where(y < hy, y, py - 1 + hy - y)

    my_x, core = xh * hx + gz // 2, gz % 2

    def members_x():
        for dx in (4, 3, 5, 2, 6, 1, 7, 0) if nxc == 8 else range(nxc):
            for dc in range(2):
                if dx or dc:
                    x, c = (my_x + dx) % nxc, (core + dc) % 2
                    yield key_of_x(x, c), ((x // hx) * half + zc, gy, 2 * (x % hx) + c)

    def members_y():
        for d in (4, 3, 5, 2, 6, 1, 7) if py == 8 else range(1, py):
            y = (gy + d) % py
            yield key_of_y(y), (gx, y, gz)

    def members_z():
        for d in range(1, half):
            z = (zc + d) % half
            yield z, (xh * half + z, gy, gz)

    def key_of_x(x, c):
        return (2 * x_rank(x) + 1 - c + npz - 2 * ox) % npz

    def key_of_y(y):
        return (y_rank(y) + py - oy) % py

    groups = ((key_of_x(my_x, core), 2 * my_x + core, npz, members_x),
              (key_of_y(gy), gy, py, members_y),
              (zc, zc, half, members_z))

    def send_go(slot):
        key, _, _, members = groups[slot]
        for other, place in members():
            when(other < key, lambda: signal_go(slot, *place))

    when(has_zu, lambda: signal(gx, gy, gz + 1))
    when(has_zl, lambda: signal(gx, gy, gz - 1))
    when(has_yu, lambda: signal(gx, gy + 1, gz))
    when(has_yl, lambda: signal(gx, gy - 1, gz))
    when(has_yu & has_zu, lambda: signal(gx, gy + 1, gz + 1))
    when(upper0, lambda: signal(half - 1, gy, gz))

    def edges(x, cond):
        when(cond & has_yu, lambda: signal(x, gy + 1, gz))
        when(cond & has_zu, lambda: signal(x, gy, gz + 1))
        when(cond & has_yu & has_zu, lambda: signal(x, gy + 1, gz + 1))

    when(first_x, lambda: signal(half, gy, gz))
    edges(gx + 1, not_last & (gx != half - 1))
    edges(half, first_x)
    def of_x(k):
        r = (k + 2 * ox) % npz
        x = x_rank(r // 2)
        return (x // hx) * half + zc, gy, 2 * (x % hx) + 1 - r % 2

    def of_y(k):
        return gx, y_rank((k + oy) % py), gz

    def of_z(k):
        return xh * half + k, gy, gz

    for (key, _, count, _), place in zip(groups, (of_x, of_y, of_z)):
        def tell(k, c, place=place):
            signal(*place(k))
            return c

        lax.fori_loop(key + 1, count, tell, 0)
    n_wait = as_int(has_zu) + as_int(has_zl) + as_int(has_yu) + as_int(has_yl) + as_int(has_yl & has_zl) + as_int(lower1 | upper0)
    n_wait = n_wait + groups[0][0] + groups[1][0] + groups[2][0]
    n_wait = n_wait + jnp.where(first_x, 0, as_int(has_yl) + as_int(has_zl) + as_int(has_yl & has_zl))

    for c in loads[6:]:
        c.start()
    with jax.named_scope("w_bar0"):
        when(lower1, lambda: pl.semaphore_wait(bar, n_wait), lambda: signal_go(GO_R, 0, gy, gz))

    zero32 = jnp.zeros((32, 128), F32)
    with jax.named_scope("w_load0"):
        for c in loads[:3]:
            c.wait()
    Uf = U.reshape((nx + 1) * 3 * 2 * 32, 128)
    with jax.named_scope("c_packz"):
        acc = zero32
        for q in range(nq):
            acc = jnp.where(lane32 == q, jnp.broadcast_to(U[q // 3, q % 3, 0, :, 0:1], (32, 128)), acc)
        ZS[...] = acc
        YS[0] = Uf[pl.ds(0, nq, stride=64), :]
    with jax.named_scope("w_load1"):
        for c in loads[3:6]:
            c.wait()
    YS[1] = Uf[pl.ds(32, nq, stride=64), :]

    with jax.named_scope("w_bar"):
        when(jnp.logical_not(lower1), lambda: pl.semaphore_wait(bar, n_wait))

    y_copy = remote(YS, YH.at[:, pl.ds(0, nq), :], S_Y, gx, gy - 1, gz)
    z_copy = remote(ZS, ZX.at[0, pl.ds(0, 32), :], S_Z, gx, gy, gz - 1)
    yz_copy = remote(ZS.at[pl.ds(0, 8), :], ZX.at[0, pl.ds(32, 8), :], S_YZ, gx, gy - 1, gz - 1)
    xm_copy = remote(U.at[0], U.at[nx], S_XM, gx - 1, gy, gz)
    xm_to_relay = remote(U.at[0], RU, S_RM, 0, gy, gz)
    xm_relay = remote(RU, U.at[nx], S_XM, half - 1, gy, gz)
    xy_copy = remote(YS.at[:, pl.ds(0, 8), :], YH.at[:, pl.ds(nq, 8), :], S_XY, gx - 1, gy - 1, gz)
    xy_to_relay = remote(YS.at[:, pl.ds(0, 8), :], RY, S_RY, 0, gy - 1, gz)
    xy_relay = remote(RY, YH.at[:, pl.ds(nq, 8), :], S_XY, half - 1, gy, gz)
    xz_copy = remote(ZS, ZX.at[1, pl.ds(0, 32), :], S_XZ, gx - 1, gy, gz - 1)
    xz_to_relay = remote(ZS, RZ.at[pl.ds(0, 32), :], S_RZ, 0, gy, gz - 1)
    xz_relay = remote(RZ.at[pl.ds(0, 32), :], ZX.at[1, pl.ds(0, 32), :], S_XZ, half - 1, gy, gz)
    xyz_copy = remote(ZS.at[pl.ds(0, 8), :], ZX.at[1, pl.ds(32, 8), :], S_XYZ, gx - 1, gy - 1, gz - 1)
    xyz_to_relay = remote(ZS.at[pl.ds(0, 8), :], RZ.at[pl.ds(32, 8), :], S_RYZ, 0, gy - 1, gz - 1)
    xyz_relay = remote(RZ.at[pl.ds(32, 8), :], ZX.at[1, pl.ds(32, 8), :], S_XYZ, half - 1, gy, gz)
    both_l, both_u = has_yl & has_zl, has_yu & has_zu

    when(has_zl, z_copy.start)
    when(has_yl & has_zl, yz_copy.start)
    when(has_yl, y_copy.start)
    when(plain_down, xm_copy.start)
    when(upper0, xm_to_relay.start)
    when(plain_down & has_yl, xy_copy.start)
    when(plain_down & has_zl, xz_copy.start)
    when(plain_down & both_l, xyz_copy.start)
    when(upper0 & has_yl, xy_to_relay.start)
    when(upper0 & has_zl, xz_to_relay.start)
    when(upper0 & both_l, xyz_to_relay.start)

    send_go(0)
    send_go(1)

    zero8 = jnp.zeros((8, 128), F32)

    @pl.when(last_x)
    def _():
        for m in range(3):
            for t in range(2):
                U[nx, m, t] = zero32
        for t in range(2):
            YH[t, nq:nq + 8, :] = zero8
            F[nx + 2, t] = zero32
            F[nx + 3, t] = zero32
        ZX[1] = jnp.zeros((40, 128), F32)

    @pl.when(first_x)
    def _():
        for t in range(2):
            F[0, t] = zero32
            F[1, t] = zero32

    @pl.when(gy == py - 1)
    def _():
        for t in range(2):
            YH[t] = jnp.zeros((nq + 8, 128), F32)
            YR[1, t] = jnp.zeros((2 * nx, 128), F32)

    @pl.when(gy == 0)
    def _():
        for t in range(2):
            YR[0, t] = jnp.zeros((2 * nx, 128), F32)

    @pl.when(gz == pz - 1)
    def _():
        ZX[0, 0:32, :] = zero32
        ZX[1, 0:32, :] = zero32
        CLr[...] = zero32

    @pl.when((gz == pz - 1) | (gy == py - 1))
    def _():
        ZX[0, 32:40, :] = zero8
        ZX[1, 32:40, :] = zero8

    @pl.when(gz == 0)
    def _():
        CRr[...] = zero32

    for t in range(2):
        yv = lax.broadcasted_iota(jnp.int32, (32, 128), 0) + gy * ny
        zv = lane32 + 128 * t + gz * 256
        INV[t] = (F32(-3.0 * (1.0 - VOID)) * taps_sum(yv, py * ny)) * taps_sum(zv, pz * 256)
    HR[...] = jnp.zeros(HR.shape, F32)

    k_load.wait()
    kv = KV[...]
    k_hi = rounded(kv)
    k_lo = kv - k_hi
    dr = lax.broadcasted_iota(jnp.int32, (24, 256), 0)
    cc = lax.broadcasted_iota(jnp.int32, (24, 256), 1)
    second = cc >= 112
    cl = jnp.where(second, cc - 112, cc)
    inside = cc < 224
    tau = cl >> 3
    in_main = cl < 96
    a_m = as_int(tau >= 6)
    a_ = jnp.where(in_main, a_m, (cl - 96) >> 3)
    mc_ = jnp.where(in_main, tau - 6 * a_m, cl & 7)
    ok = inside & (mc_ < 6)
    d0 = 8 * (mc_ >> 1) + 4 * a_ + (mc_ & 1)
    kb = []
    for b in range(2):
        pick = ok & (dr == d0 + 2 * b)
        b_hi = jnp.where(pick & jnp.logical_not(second), F32(1), F32(0))
        b_lo = jnp.where(pick & second, F32(1), F32(0))
        kb.append(jnp.dot(k_hi, b_hi, preferred_element_type=F32) + jnp.dot(k_lo, b_lo, preferred_element_type=F32))
    cy = lax.broadcasted_iota(jnp.int32, (16, 256), 1)
    yy = lax.broadcasted_iota(jnp.int32, (16, 256), 0) & 7
    cy = jnp.where(cy >= 112, cy - 112, cy)
    rr = jnp.where(cy < 96, cy & 7, 8)
    m0, m1 = rr == yy, rr == yy + 1
    for d in range(0, 24, 2):
        r0, r1 = (jnp.concatenate([jnp.broadcast_to(kb[b][d + k:d + k + 1, :], (8, 256)) for k in range(2)], axis=0)
                  for b in range(2))
        L[8 * d:8 * d + 16, :] = jnp.where(m0, r0, jnp.where(m1, r1, F32(0))).astype(jnp.bfloat16)

    def store_pair(p, m, t, x0, x1):
        for j in range(4):
            x = jnp.concatenate([x0[8 * j:8 * j + 8], x1[8 * j:8 * j + 8]], axis=0)
            h = x.astype(jnp.bfloat16)
            UH[p, m, t, j] = h
            g = 2.0 * x - h.astype(F32)
            G[0, p, m, t, 8 * j:8 * j + 8, :] = g[0:8]
            G[1, p, m, t, 8 * j:8 * j + 8, :] = g[8:16]
            if j > 0:
                HR[p, t, 8 * j - 8 + 2 * m:8 * j - 7 + 2 * m, :] = x0[8 * j:8 * j + 1]
                HR[p, t, 8 * j - 7 + 2 * m:8 * j - 6 + 2 * m, :] = x1[8 * j:8 * j + 1]

    def shifted(p, m, t, zx):
        s1 = pltpu.roll(U[p, m, 1], 127, 1)
        if t == 1:
            return jnp.where(lane32 == 127, zx, s1)
        return jnp.where(lane32 == 127, s1, pltpu.roll(U[p, m, 0], 127, 1))

    def prep(p, t, z_row=None, first=0):
        for m in range(3):
            zx = None if t == 0 else pltpu.roll(z_row, 127 - (3 * p + m - first), 1)
            store_pair(p, m, t, U[p, m, t], shifted(p, m, t, zx))

    Gf = G.reshape(2 * (nx + 1) * 3 * 2 * 40, 128)
    HRf = HR.reshape((nx + 1) * 2 * 32, 128)

    def halo_rows(first, count, zx_row, planes):
        lanes = lax.broadcasted_iota(jnp.int32, (count, 128), 1)
        rows = lax.broadcasted_iota(jnp.int32, (count, 128), 0)
        nxt = jnp.sum(jnp.where(lanes == rows, jnp.broadcast_to(zx_row, (count, 128)), 0.0), axis=1, keepdims=True)
        u0, u1 = YH[0, first:first + count, :], YH[1, first:first + count, :]
        s0, s1 = pltpu.roll(u0, 127, 1), pltpu.roll(u1, 127, 1)
        v0 = jnp.where(lanes == 127, s1, s0)
        v1 = jnp.where(lanes == 127, jnp.broadcast_to(nxt, (count, 128)), s1)
        for c, pair in enumerate(((u0, u1), (v0, v1))):
            for t in range(2):
                HY[c, t, first:first + count, :] = pair[t]
                GY[c, t, first:first + count, :] = 2.0 * pair[t] - rounded(pair[t])
        for c in range(2):
            for t in range(2):
                n = 3 * planes
                at = ((c * (nx + 1) + first // 3) * 6 + t) * 40 + 32
                Gf[pl.ds(at, n, stride=80), :] = GY[c, t, first:first + n, :]
                for m in range(3):
                    at = ((first // 3) * 2 + t) * 32 + 24 + 2 * m + c
                    if planes == 1:
                        HRf[at:at + 1, :] = HY[c, t, first + m:first + m + 1, :]
                    else:
                        HRf[pl.ds(at, planes, stride=64), :] = HY[c, t, pl.ds(first + m, planes, stride=3), :]

    def pairs(todo, acc):
        comp, vol = acc
        for pair in todo:
            cols = []
            for i, j, t in pair:
                tiles = [UH[i + a, m, t, j] for a in range(2) for m in range(3)]
                tiles.append(jnp.concatenate(
                    [HR[i, t, 8 * j:8 * j + 8, :], HR[i + 1, t, 8 * j:8 * j + 8, :]], axis=0).astype(jnp.bfloat16))
                cols.append(jnp.concatenate(tiles, axis=0))
            rhs = jnp.concatenate(cols, axis=1)
            rhs = jnp.concatenate([rhs, rhs], axis=0)
            prod = jnp.dot(L[:, 0:224], rhs, preferred_element_type=F32)
            for side, (i, j, t) in enumerate(pair):
                r0 = 8 * j
                e = None
                for d in range(24):
                    m, a, b, c = d // 8, (d // 4) % 2, (d // 2) % 2, d % 2
                    term = prod[8 * d:8 * d + 8, 128 * side:128 * side + 128] * G[c, i + a, m, t, pl.ds(r0 + b, 8), :]
                    e = term if e is None else e + term
                rho = R[i, t, r0:r0 + 8, :]
                r2 = rho * rho
                comp = comp + (VOID + (r2 * rho) * (1.0 - VOID)) * e
                vol = vol + rho
                W[i, t, r0:r0 + 8, :] = (r2 * e) * (INV[t, r0:r0 + 8, :] * taps_sum(gx * nx + i, px * nx))
        return comp, vol

    def half_region(t, z_row, acc):
        for p in range(3):
            prep(p, t, z_row)
        for i in range(0, nx - 2, 2):
            for p in (i + 3, i + 4):
                if p < nx:
                    prep(p, t, z_row)
            acc = pairs([((i, 0, t), (i, 1, t)), ((i + 1, 0, t), (i + 1, 1, t)), ((i, 2, t), (i + 1, 2, t))], acc)
        return acc

    for c in loads[6:8]:
        c.wait()
    with jax.named_scope("c_main0"):
        acc = half_region(0, None, (zero8, zero8))
    wait("w_z", (has_zu, z_copy.wait_recv))
    with jax.named_scope("c_main1"):
        acc = half_region(1, ZX[0, 0:32, :], acc)
        i = nx - 2
        acc = pairs([((i, 0, 0), (i, 1, 0)), ((i, 0, 1), (i, 1, 1)), ((i, 2, 0), (i, 2, 1))], acc)
    wait("w_yz", (both_u, yz_copy.wait_recv))
    wait("w_y", (has_yu, y_copy.wait_recv))
    with jax.named_scope("c_halo"):
        halo_rows(0, nq, ZX[0, 32:33, :], nx)
    with jax.named_scope("c_main2"):
        acc = lax.fori_loop(0, nx - 1, lambda i, a: pairs([((i, 3, 0), (i, 3, 1))], a), acc, unroll=UNROLL_LAST)

    def relay():
        pl.semaphore_wait(go.at[GO_R], 1)
        when(has_yu, xy_to_relay.wait_recv, xy_relay.start)
        when(has_zu, xz_to_relay.wait_recv, xz_relay.start)
        when(both_u, xyz_to_relay.wait_recv, xyz_relay.start)
        xm_to_relay.wait_recv()
        xm_relay.start()

    wait("w_xm", (not_last, xm_copy.wait_recv))
    wait("w_xe", (not_last & has_yu, xy_copy.wait_recv), (not_last & has_zu, xz_copy.wait_recv),
         (not_last & both_u, xyz_copy.wait_recv))
    with jax.named_scope("c_last"):
        prep(nx, 0)
        prep(nx, 1, ZX[1, 0:32, :], 3 * nx)
        halo_rows(nq, 8, ZX[1, 32:33, :], 1)
        i = nx - 1
        comp, vol = pairs([((i, j, 0), (i, j, 1)) for j in range(4)], acc)

    row_of = zc * py + gy

    def row_copy(buf, me, sems, place):
        return pltpu.make_async_remote_copy(
            src_ref=buf.at[me], dst_ref=buf.at[me], send_sem=sems[0], recv_sem=sems[1],
            device_id=dev(*place), device_id_type=MESH)

    def wait_rows(buf, count, sem):
        part = buf.at[pl.ds(0, count)]
        pltpu.make_async_copy(part, part, sem).wait()

    def add_up(rows):
        while len(rows) > 1:
            rows = [a + b for a, b in zip(rows[::2], rows[1::2])] + ([rows[-1]] if len(rows) % 2 else [])
        return rows[0]

    def x_copy(place):
        return row_copy(A1, groups[0][1], (ar_send.at[0], ar_recv.at[0]), place)

    def y_copy_of(place):
        return row_copy(A2, row_of, (ar_send.at[1], ar_recv.at[1]), place)

    def down_copy(z, y):
        return row_copy(A2, row_of, (down_send.at[z], down_recv.at[zc]), (xh * half + z, y, gz))

    def up_copy(z):
        return row_copy(A3, zc, (up_send.at[z], up_recv.at[zc]), (xh * half + z, gy, gz))

    def when_any(number, slot):
        when(number > 0, lambda: pl.semaphore_wait(go.at[slot], number))

    key_y = groups[1][0]

    lane1 = lax.broadcasted_iota(jnp.int32, (1, 128), 1)
    comp_all = jnp.sum(jnp.sum(comp, axis=0, keepdims=True), axis=1, keepdims=True)
    vol_all = jnp.sum(jnp.sum(vol, axis=0, keepdims=True), axis=1, keepdims=True)
    A1[groups[0][1]] = jnp.where(lane1 == 0, jnp.broadcast_to(comp_all, (1, 128)), jnp.broadcast_to(vol_all, (1, 128)))
    with jax.named_scope("w_go0"):
        when_any(npz - 1 - groups[0][0], 0)
    for _, place in members_x():
        x_copy(place).start()
    when(zc > 0, lambda: signal_go(GO_U, gx - 1, gy, gz))

    for t in range(2):
        zr = lax.broadcasted_iota(jnp.int32, (256, 128), 0)
        zl = lax.broadcasted_iota(jnp.int32, (256, 128), 1) + 128 * t
        T[:, 128 * t:128 * t + 128] = jnp.maximum(3 - jnp.abs(zr - zl), 0).astype(F32).astype(jnp.bfloat16)

    with jax.named_scope("c_packw"):
        lo, hi = zero32, zero32
        for p in range(nx):
            w0, w1 = W[p, 0], W[p, 1]
            for k in range(2):
                lo = jnp.where(lane32 == 2 * p + k, jnp.broadcast_to(w0[:, k:k + 1], (32, 128)), lo)
                hi = jnp.where(lane32 == 2 * p + k, jnp.broadcast_to(w1[:, 126 + k:127 + k], (32, 128)), hi)
        even = (lane32 & 1) == 0
        CL[...] = jnp.where(even, lo, lo + 2.0 * pltpu.roll(lo, 1, 1))
        CR[...] = jnp.where(even, hi + 2.0 * pltpu.roll(hi, 127, 1), hi)
    zl_copy = remote(CL, CLr, S_ZL, gx, gy, gz - 1)
    zr_copy = remote(CR, CRr, S_ZR, gx, gy, gz + 1)
    when(has_zl, zl_copy.start)
    when(has_zu, zr_copy.start)

    def filter_z(g, carry):
        w = jnp.concatenate([jnp.concatenate([W[4 * g + k, 0], W[4 * g + k, 1]], axis=1) for k in range(4)], axis=0)
        w_hi = w.astype(jnp.bfloat16)
        w_lo = (w - w_hi.astype(F32)).astype(jnp.bfloat16)
        z = jnp.dot(w_hi, T[...], preferred_element_type=F32) + jnp.dot(w_lo, T[...], preferred_element_type=F32)
        for k in range(4):
            for t in range(2):
                Z[4 * g + k, t, 8:40, :] = z[32 * k:32 * k + 32, 128 * t:128 * t + 128]
        return carry

    with jax.named_scope("c_fz"):
        lax.fori_loop(0, nx // 4, filter_z, 0, unroll=True)

    with jax.named_scope("w_go1"):
        when_any(py - 1 - key_y, 1)
    for other, place in members_y():
        when(other > key_y, lambda: signal_go(GO_T, *place))
    send_go(2)
    wait("w_relay", (first_x, relay))
    wait("w_wz", (has_zu, zl_copy.wait_recv), (has_zl, zr_copy.wait_recv))
    with jax.named_scope("c_fixz"):
        left, right = CRr[...], CLr[...]
        for p in range(nx):
            Z[p, 0, 8:40, :] += jnp.where(lane32 < 2, pltpu.roll(left, (128 - 2 * p) % 128, 1), 0.0)
            Z[p, 1, 8:40, :] += jnp.where(lane32 >= 126, pltpu.roll(right, 126 - 2 * p, 1), 0.0)

    Zf = Z.reshape(nx * 2 * 48, 128)
    for t in range(2):
        for r in range(2):
            YS2[0, t, r * nx:(r + 1) * nx, :] = Zf[pl.ds(48 * t + 8 + r, nx, stride=96), :]
            YS2[1, t, r * nx:(r + 1) * nx, :] = Zf[pl.ds(48 * t + 38 + r, nx, stride=96), :]
    yd_copy = remote(YS2.at[0], YR.at[1], S_YD, gx, gy - 1, gz)
    yu_copy = remote(YS2.at[1], YR.at[0], S_YU, gx, gy + 1, gz)
    when(has_yl, yd_copy.start)
    when(has_yu, yu_copy.start)

    def second_stage():
        with jax.named_scope("w_ar0"):
            wait_rows(A1, npz - 1, ar_recv.at[0])
        A2[row_of] = add_up([A1[k] for k in range(npz)])
        with jax.named_scope("w_got"):
            when_any(key_y, GO_T)
        for z in range(half - 1):
            @pl.when(z < zc)
            def _():
                for dy in range(py):
                    down_copy(z, (gy + hy + dy) % py).start()
        for _, place in members_y():
            y_copy_of(place).start()

    layers_first = lower1 & (gy == 0)
    when(jnp.logical_not(layers_first), second_stage)

    wait("w_wy", (has_yu, yd_copy.wait_recv), (has_yl, yu_copy.wait_recv))
    for t in range(2):
        for r in range(2):
            Zf[pl.ds(48 * t + 6 + r, nx, stride=96), :] = YR[0, t, r * nx:(r + 1) * nx, :]
            Zf[pl.ds(48 * t + 40 + r, nx, stride=96), :] = YR[1, t, r * nx:(r + 1) * nx, :]

    def filter_y(p, carry):
        for t in range(2):
            z = [Z[p, t, 6 + d:38 + d, :] for d in range(5)]
            F[p + 2, t] = 3.0 * z[2] + 2.0 * (z[1] + z[3]) + (z[0] + z[4])
        return carry

    with jax.named_scope("c_fy"):
        lax.fori_loop(0, nx, filter_y, 0, unroll=2)

    xd_copy = remote(F.at[pl.ds(2, 2)], F.at[pl.ds(nx + 2, 2)], S_XD, gx - 1, gy, gz)
    xd_to_relay = remote(F.at[pl.ds(2, 2)], RF, S_RF, 0, gy, gz)
    xd_relay = remote(RF, F.at[pl.ds(nx + 2, 2)], S_XD, half - 1, gy, gz)
    xu_copy = remote(F.at[pl.ds(nx, 2)], F.at[pl.ds(0, 2)], S_XU, gx + 1, gy, gz)
    when(plain_down, xd_copy.start)
    when(upper0, xd_to_relay.start)
    when(zc < half - 1, lambda: pl.semaphore_wait(go.at[GO_U], 1))
    when(not_last, xu_copy.start)
    when(layers_first, second_stage)

    def filter_x(p, carry):
        for t in range(2):
            f = [F[p + d, t] for d in range(5)]
            out[p, :, 128 * t:128 * t + 128] = 3.0 * f[2] + 2.0 * (f[1] + f[3]) + (f[0] + f[4])
        return carry

    wait("w_frelay", (first_x, xd_to_relay.wait_recv, xd_relay.start))
    with jax.named_scope("c_fx"):
        lax.fori_loop(2, nx - 2, filter_x, 0, unroll=2)
    with jax.named_scope("w_ar1"):
        wait_rows(A2, py - 1, ar_recv.at[1])
    A3[zc] = add_up([A2[zc * py + k] for k in range(py)])
    with jax.named_scope("w_go2"):
        when_any(half - 1 - zc, 2)
    for z in range(1, half):
        when(z > zc, up_copy(z).start)

    wait("w_fd", (not_last, xd_copy.wait_recv))
    for p in (nx - 2, nx - 1):
        filter_x(p, 0)
    wait("w_fu", (not_first, xu_copy.wait_recv))
    for p in (0, 1):
        filter_x(p, 0)

    with jax.named_scope("w_sends"):
        when(has_yl, y_copy.wait_send, yd_copy.wait_send)
        when(has_zl, z_copy.wait_send, zl_copy.wait_send)
        when(has_yl & has_zl, yz_copy.wait_send)
        when(has_zu, zr_copy.wait_send)
        when(has_yu, yu_copy.wait_send)
        when(plain_down, xm_copy.wait_send, xd_copy.wait_send)
        when(plain_down & has_yl, xy_copy.wait_send)
        when(plain_down & has_zl, xz_copy.wait_send)
        when(plain_down & both_l, xyz_copy.wait_send)
        when(upper0, xm_to_relay.wait_send, xd_to_relay.wait_send)
        when(upper0 & has_yl, xy_to_relay.wait_send)
        when(upper0 & has_zl, xz_to_relay.wait_send)
        when(upper0 & both_l, xyz_to_relay.wait_send)
        when(first_x, xm_relay.wait_send, xd_relay.wait_send)
        when(first_x & has_yu, xy_relay.wait_send)
        when(first_x & has_zu, xz_relay.wait_send)
        when(first_x & both_u, xyz_relay.wait_send)
        when(not_last, xu_copy.wait_send)
        wait_rows(A1, npz - 1, ar_send.at[0])
        wait_rows(A2, py - 1, ar_send.at[1])
        for z in range(half):
            when(z < zc, lambda: wait_rows(A2, py, down_send.at[z]))
            when(z > zc, lambda: wait_rows(A3, 1, up_send.at[z]))

    def add_upper(z, c):
        wait_rows(A2, py, down_recv.at[z])
        A3[z] = add_up([A2[z * py + k] for k in range(py)])
        return c

    def add_lower(z, c):
        wait_rows(A3, 1, up_recv.at[z])
        return c

    with jax.named_scope("w_ar2"):
        lax.fori_loop(0, zc, add_lower, 0)
        lax.fori_loop(zc + 1, half, add_upper, 0)
    total = add_up([A3[z] for z in range(half)])
    count = F32(px * nx) * F32(py * ny) * F32(pz * 256)
    sums[...] = jnp.broadcast_to(total / count, (8, 128))


def finish(out_ref, sums_ref, filtered, comp, vol, c_ref, v_ref, sem):
    copies = [pltpu.make_async_copy(out_ref, filtered, sem.at[0])]
    copies[0].start()
    c_ref[...] = sums_ref[0:1, 0:1]
    v_ref[...] = sums_ref[0:1, 1:2]
    for k, (src, dst) in enumerate(((c_ref, comp), (v_ref, vol))):
        copies.append(pltpu.make_async_copy(src, dst, sem.at[1 + k]))
        copies[-1].start()
    for c in copies:
        c.wait()


def on_device(displacement, density, stiffness):
    px, py, pz = lax.axis_size("gx"), lax.axis_size("gy"), lax.axis_size("gz")
    nx, ny, nz = density.shape
    nq = 3 * nx
    vm = lambda *shape: pltpu.VMEM(shape, F32)
    out, sums = pl.pallas_call(
        functools.partial(kernel, nx, ny, px, py, pz),
        out_shape=(jax.ShapeDtypeStruct((nx, ny, nz), F32), jax.ShapeDtypeStruct((8, 128), F32)),
        in_specs=[pl.BlockSpec(memory_space=pltpu.HBM)] * 3,
        out_specs=(pl.BlockSpec(memory_space=pltpu.VMEM), pl.BlockSpec(memory_space=pltpu.VMEM)),
        scratch_shapes=[
            vm(nx + 1, 3, 2, 32, 128),
            pltpu.VMEM((nx + 1, 3, 2, 4, 16, 128), jnp.bfloat16),
            vm(2, nx + 1, 3, 2, 40, 128),
            vm(nx + 1, 2, 32, 128),
            vm(nx, 2, 32, 128),
            vm(nx, 2, 32, 128),
            vm(nx, 2, 48, 128),
            vm(nx + 4, 2, 32, 128),
            pltpu.VMEM((256, 256), jnp.bfloat16),
            pltpu.VMEM((192, 256), jnp.bfloat16),
            vm(24, 24),
            vm(2, 32, 128),
            vm(2, nq, 128),
            vm(2, nq + 8, 128),
            vm(2, 2, nq + 8, 128),
            vm(2, 2, nq + 8, 128),
            vm(32, 128),
            vm(2, 40, 128),
            vm(3, 2, 32, 128),
            vm(2, 8, 128),
            vm(40, 128),
            vm(32, 128), vm(32, 128), vm(32, 128), vm(32, 128),
            vm(2, 2, 2 * nx, 128),
            vm(2, 2, 2 * nx, 128),
            vm(2, 2, 32, 128),
            vm(2 * pz, 1, 128), vm(py * px // 2, 1, 128), vm(px // 2, 1, 128),
            pltpu.SemaphoreType.DMA((9,)),
            pltpu.SemaphoreType.DMA((N_SEM,)),
            pltpu.SemaphoreType.DMA((N_SEM,)),
            pltpu.SemaphoreType.DMA((2,)),
            pltpu.SemaphoreType.DMA((2,)),
            pltpu.SemaphoreType.DMA((px // 2,)),
            pltpu.SemaphoreType.DMA((px // 2,)),
            pltpu.SemaphoreType.DMA((px // 2,)),
            pltpu.SemaphoreType.DMA((px // 2,)),
            pltpu.SemaphoreType.REGULAR((6,)),
        ],
        compiler_params=pltpu.CompilerParams(collective_id=0, has_side_effects=True, vmem_limit_bytes=56_000_000),
    )(displacement, density, pltpu.with_memory_space_constraint(stiffness, pltpu.HBM))
    vmem = pl.BlockSpec(memory_space=pltpu.VMEM)
    out, comp, vol = pl.pallas_call(
        finish,
        out_shape=(jax.ShapeDtypeStruct((nx, ny, nz), F32), jax.ShapeDtypeStruct((1, 1), F32), jax.ShapeDtypeStruct((1, 1), F32)),
        in_specs=[vmem, vmem],
        out_specs=(pl.BlockSpec(memory_space=pltpu.HBM),) * 3,
        scratch_shapes=[pltpu.VMEM((1, 1), F32), pltpu.VMEM((1, 1), F32), pltpu.SemaphoreType.DMA((3,))],
        compiler_params=pltpu.CompilerParams(vmem_limit_bytes=4 << 20),
    )(out, sums)
    return out, comp.reshape(()), vol.reshape(())


def solution(mesh):
    return jax.shard_map(
        on_device,
        mesh=mesh,
        in_specs=(P(None, "gx", "gy", "gz"), P("gx", "gy", "gz"), P()),
        out_specs=(P("gx", "gy", "gz"), P(), P()),
        check_vma=False,
    )
```

```python
import functools

import jax
import jax.numpy as jnp
from jax import lax
from jax.experimental import pallas as pl
from jax.experimental.pallas import tpu as pltpu
from jax.sharding import PartitionSpec as P

VOID = 0.001
MESH = pl.DeviceIdType.MESH
F32 = jnp.float32

S_Y, S_Z, S_YZ, S_XM, S_XY, S_XZ, S_RM, S_RY, S_RZ = range(9)
S_ZL, S_ZR, S_YD, S_YU, S_XD, S_XU, S_RF = range(9, 16)
S_XYZ, S_RYZ = 16, 17
N_SEM = 18
GO_U, GO_R, GO_T, GO_V = 3, 4, 5, 6
UNROLL_LAST = 15


def rounded(v):
    return v.astype(jnp.bfloat16).astype(F32)


def taps_sum(position, extent):
    low = jnp.minimum(position, extent - 1 - position)
    return jnp.where(low == 0, F32(1 / 6), jnp.where(low == 1, F32(1 / 8), F32(1 / 9)))


def kernel(nx, ny, px, py, pz,
           disp, dens, stiff,
           out, sums,
           U, UH, G, HR, R, W, Z, F, T, L, KV, INV,
           YS, YH, HY, GY, ZS, ZX, RU, RY, RZ,
           CL, CR, CLr, CRr, YS2, YR, RF, A1, A2, A3,
           load_sem, send_sem, recv_sem, ar_send, ar_recv, down_send, down_recv, up_send, up_recv, go):
    gx, gy, gz = lax.axis_index("gx"), lax.axis_index("gy"), lax.axis_index("gz")
    half = px // 2
    xh, zc = gx // half, gx % half
    lane32 = lax.broadcasted_iota(jnp.int32, (32, 128), 1)
    nq = 3 * nx
    npz = 2 * pz

    def dev(x, y, z):
        return {"gx": x, "gy": y, "gz": z}

    def remote(src, dst, slot, x, y, z):
        return pltpu.make_async_remote_copy(
            src_ref=src, dst_ref=dst, send_sem=send_sem.at[slot], recv_sem=recv_sem.at[slot],
            device_id=dev(x, y, z), device_id_type=MESH)

    def when(cond, *actions):
        @pl.when(cond)
        def _():
            for act in actions:
                act()

    def wait(name, *pairs):
        with jax.named_scope(name):
            for cond, *actions in pairs:
                when(cond, *actions)

    loads = []
    for t in range(2):
        for m in range(3):
            loads.append(pltpu.make_async_copy(
                disp.at[m, :, :, pl.ds(128 * t, 128)], U.at[pl.ds(0, nx), m, t], load_sem.at[3 * t + m]))
    for t in range(2):
        loads.append(pltpu.make_async_copy(dens.at[:, :, pl.ds(128 * t, 128)], R.at[:, t], load_sem.at[6 + t]))
    k_load = pltpu.make_async_copy(stiff, KV, load_sem.at[8])
    for c in loads[:6] + [k_load]:
        c.start()

    has_yl, has_yu = gy > 0, gy < py - 1
    has_zl, has_zu = gz > 0, gz < pz - 1
    last_x, first_x, upper0, lower1 = gx == px - 1, gx == 0, gx == half, gx == half - 1
    not_last, not_first = gx < px - 1, gx > 0
    plain_down = not_first & (gx != half)

    bar = pltpu.get_barrier_semaphore()

    def signal(x, y, z):
        pl.semaphore_signal(bar, inc=1, device_id=dev(x, y, z), device_id_type=MESH)

    def signal_go(slot, x, y, z):
        pl.semaphore_signal(go.at[slot], inc=1, device_id=dev(x, y, z), device_id_type=MESH)

    def as_int(c):
        return c.astype(jnp.int32)

    nxc, hx, hy = pz, pz // 2, py // 2
    at_origin = lambda c: jnp.where(c, 1, 0)
    ox = at_origin((gy == 0) & (zc == 0))
    oy = at_origin((gx == 0) & (gz == 0))

    def x_rank(x):
        return jnp.where(x < hx, x, nxc - 1 + hx - x)

    def y_rank(y):
        return jnp.where(y < hy, y, py - 1 + hy - y)

    my_x, core = xh * hx + gz // 2, gz % 2

    def members_x():
        for dx in (4, 3, 5, 2, 6, 1, 7, 0) if nxc == 8 else range(nxc):
            for dc in range(2):
                if dx or dc:
                    x, c = (my_x + dx) % nxc, (core + dc) % 2
                    yield key_of_x(x, c), ((x // hx) * half + zc, gy, 2 * (x % hx) + c)

    def members_y():
        for d in (4, 3, 5, 2, 6, 1, 7) if py == 8 else range(1, py):
            y = (gy + d) % py
            yield key_of_y(y), (gx, y, gz)

    def members_z():
        for d in range(1, half):
            z = (zc + d) % half
            yield z, (xh * half + z, gy, gz)

    def key_of_x(x, c):
        return (2 * x_rank(x) + 1 - c + npz - 2 * ox) % npz

    def key_of_y(y):
        return (y_rank(y) + py - oy) % py

    groups = ((key_of_x(my_x, core), 2 * my_x + core, npz, members_x),
              (key_of_y(gy), gy, py, members_y),
              (zc, zc, half, members_z))

    def send_go(slot):
        key, _, _, members = groups[slot]
        for other, place in members():
            when(other < key, lambda: signal_go(slot, *place))

    when(has_zu, lambda: signal(gx, gy, gz + 1))
    when(has_zl, lambda: signal(gx, gy, gz - 1))
    when(has_yu, lambda: signal(gx, gy + 1, gz))
    when(has_yu & has_zu, lambda: signal(gx, gy + 1, gz + 1))
    when(upper0, lambda: signal(half - 1, gy, gz))

    def edges(x, cond):
        when(cond & has_yu, lambda: signal(x, gy + 1, gz))
        when(cond & has_zu, lambda: signal(x, gy, gz + 1))
        when(cond & has_yu & has_zu, lambda: signal(x, gy + 1, gz + 1))

    when(first_x, lambda: signal(half, gy, gz))
    edges(gx + 1, not_last & (gx != half - 1))
    edges(half, first_x & ((gy > 0) | (gz > 0)))
    skip_y, skip_z, skip_yz = (upper0 & (gy == y) & (gz == z) for y, z in ((1, 0), (0, 1), (1, 1)))
    at_corner = upper0 & (gy == 0) & (gz == 0)
    when((gx == half + half // 2 - 1) & (gy < 2) & (gz < 2) & (gy + gz > 0), lambda: signal(half, gy, gz))
    def of_x(k):
        r = (k + 2 * ox) % npz
        x = x_rank(r // 2)
        return (x // hx) * half + zc, gy, 2 * (x % hx) + 1 - r % 2

    def of_y(k):
        return gx, y_rank((k + oy) % py), gz

    def of_z(k):
        return xh * half + k, gy, gz

    for (key, _, count, _), place in zip(groups, (of_x, of_y, of_z)):
        def tell(k, c, place=place):
            signal(*place(k))
            return c

        lax.fori_loop(key + 1, count, tell, 0)
    n_wait = as_int(has_zu) + as_int(has_zl) + as_int(has_yl) + as_int(has_yl & has_zl) + as_int(lower1 | upper0)
    n_wait = n_wait + groups[0][0] + groups[1][0] + groups[2][0]
    n_wait = n_wait + jnp.where(first_x, 0, as_int(has_yl) + as_int(has_zl) + as_int(has_yl & has_zl))

    for c in loads[6:]:
        c.start()
    with jax.named_scope("w_bar0"):
        when(lower1, lambda: pl.semaphore_wait(bar, n_wait), lambda: signal_go(GO_R, 0, gy, gz))

    zero32 = jnp.zeros((32, 128), F32)
    with jax.named_scope("w_load0"):
        for c in loads[:3]:
            c.wait()
    Uf = U.reshape((nx + 1) * 3 * 2 * 32, 128)
    with jax.named_scope("c_packz"):
        acc = zero32
        for q in range(nq):
            acc = jnp.where(lane32 == q, jnp.broadcast_to(U[q // 3, q % 3, 0, :, 0:1], (32, 128)), acc)
        ZS[...] = acc
        YS[0] = Uf[pl.ds(0, nq, stride=64), :]
    with jax.named_scope("w_load1"):
        for c in loads[3:6]:
            c.wait()
    YS[1] = Uf[pl.ds(32, nq, stride=64), :]

    with jax.named_scope("w_bar"):
        when(jnp.logical_not(lower1), lambda: pl.semaphore_wait(bar, n_wait))

    y_copy = remote(YS, YH.at[:, pl.ds(0, nq), :], S_Y, gx, gy - 1, gz)
    z_copy = remote(ZS, ZX.at[0, pl.ds(0, 32), :], S_Z, gx, gy, gz - 1)
    yz_copy = remote(ZS.at[pl.ds(0, 8), :], ZX.at[0, pl.ds(32, 8), :], S_YZ, gx, gy - 1, gz - 1)
    xm_copy = remote(U.at[0], U.at[nx], S_XM, gx - 1, gy, gz)
    xm_to_relay = remote(U.at[0], RU, S_RM, 0, gy, gz)
    xm_relay = remote(RU, U.at[nx], S_XM, half - 1, gy, gz)
    xy_copy = remote(YS.at[:, pl.ds(0, 8), :], YH.at[:, pl.ds(nq, 8), :], S_XY, gx - 1, gy - 1, gz)
    xy_to_relay = remote(YS.at[:, pl.ds(0, 8), :], RY, S_RY, 0, gy - 1, gz)
    xy_relay = remote(RY, YH.at[:, pl.ds(nq, 8), :], S_XY, half - 1, gy, gz)
    xz_copy = remote(ZS, ZX.at[1, pl.ds(0, 32), :], S_XZ, gx - 1, gy, gz - 1)
    xz_to_relay = remote(ZS, RZ.at[pl.ds(0, 32), :], S_RZ, 0, gy, gz - 1)
    xz_relay = remote(RZ.at[pl.ds(0, 32), :], ZX.at[1, pl.ds(0, 32), :], S_XZ, half - 1, gy, gz)
    xyz_copy = remote(ZS.at[pl.ds(0, 8), :], ZX.at[1, pl.ds(32, 8), :], S_XYZ, gx - 1, gy - 1, gz - 1)
    xyz_to_relay = remote(ZS.at[pl.ds(0, 8), :], RZ.at[pl.ds(32, 8), :], S_RYZ, 0, gy - 1, gz - 1)
    xyz_relay = remote(RZ.at[pl.ds(32, 8), :], ZX.at[1, pl.ds(32, 8), :], S_XYZ, half - 1, gy, gz)
    both_l, both_u = has_yl & has_zl, has_yu & has_zu

    when(has_zl, z_copy.start)
    when(has_yl & has_zl, yz_copy.start)
    when(has_yl, y_copy.start)
    when(plain_down, xm_copy.start)
    when(upper0, xm_to_relay.start)
    when(plain_down & has_yl, xy_copy.start)
    when(plain_down & has_zl, xz_copy.start)
    when(plain_down & both_l, xyz_copy.start)
    no = jnp.logical_not
    when(upper0 & has_yl & no(skip_y), xy_to_relay.start)
    when(upper0 & has_zl & no(skip_z), xz_to_relay.start)
    when(upper0 & both_l & no(skip_yz), xyz_to_relay.start)
    xy_corner = remote(YH.at[:, pl.ds(0, 8), :], RY, S_RY, 0, gy, gz)
    xz_corner = remote(ZX.at[0, pl.ds(0, 32), :], RZ.at[pl.ds(0, 32), :], S_RZ, 0, gy, gz)
    xyz_corner = remote(ZX.at[0, pl.ds(32, 8), :], RZ.at[pl.ds(32, 8), :], S_RYZ, 0, gy, gz)

    when(has_yl, lambda: signal_go(GO_V, gx, gy - 1, gz))
    send_go(0)
    send_go(1)

    zero8 = jnp.zeros((8, 128), F32)

    @pl.when(last_x)
    def _():
        for m in range(3):
            for t in range(2):
                U[nx, m, t] = zero32
        for t in range(2):
            YH[t, nq:nq + 8, :] = zero8
            F[nx + 2, t] = zero32
            F[nx + 3, t] = zero32
        ZX[1] = jnp.zeros((40, 128), F32)

    @pl.when(first_x)
    def _():
        for t in range(2):
            F[0, t] = zero32
            F[1, t] = zero32

    @pl.when(gy == py - 1)
    def _():
        for t in range(2):
            YH[t] = jnp.zeros((nq + 8, 128), F32)
            YR[1, t] = jnp.zeros((2 * nx, 128), F32)

    @pl.when(gy == 0)
    def _():
        for t in range(2):
            YR[0, t] = jnp.zeros((2 * nx, 128), F32)

    @pl.when(gz == pz - 1)
    def _():
        ZX[0, 0:32, :] = zero32
        ZX[1, 0:32, :] = zero32
        CLr[...] = zero32

    @pl.when((gz == pz - 1) | (gy == py - 1))
    def _():
        ZX[0, 32:40, :] = zero8
        ZX[1, 32:40, :] = zero8

    @pl.when(gz == 0)
    def _():
        CRr[...] = zero32

    for t in range(2):
        yv = lax.broadcasted_iota(jnp.int32, (32, 128), 0) + gy * ny
        zv = lane32 + 128 * t + gz * 256
        INV[t] = (F32(-3.0 * (1.0 - VOID)) * taps_sum(yv, py * ny)) * taps_sum(zv, pz * 256)
    HR[...] = jnp.zeros(HR.shape, F32)

    k_load.wait()
    kv = KV[...]
    k_hi = rounded(kv)
    k_lo = kv - k_hi
    dr = lax.broadcasted_iota(jnp.int32, (24, 256), 0)
    cc = lax.broadcasted_iota(jnp.int32, (24, 256), 1)
    second = cc >= 112
    cl = jnp.where(second, cc - 112, cc)
    inside = cc < 224
    tau = cl >> 3
    in_main = cl < 96
    a_m = as_int(tau >= 6)
    a_ = jnp.where(in_main, a_m, (cl - 96) >> 3)
    mc_ = jnp.where(in_main, tau - 6 * a_m, cl & 7)
    ok = inside & (mc_ < 6)
    d0 = 8 * (mc_ >> 1) + 4 * a_ + (mc_ & 1)
    kb = []
    for b in range(2):
        pick = ok & (dr == d0 + 2 * b)
        b_hi = jnp.where(pick & jnp.logical_not(second), F32(1), F32(0))
        b_lo = jnp.where(pick & second, F32(1), F32(0))
        kb.append(jnp.dot(k_hi, b_hi, preferred_element_type=F32) + jnp.dot(k_lo, b_lo, preferred_element_type=F32))
    cy = lax.broadcasted_iota(jnp.int32, (16, 256), 1)
    yy = lax.broadcasted_iota(jnp.int32, (16, 256), 0) & 7
    cy = jnp.where(cy >= 112, cy - 112, cy)
    rr = jnp.where(cy < 96, cy & 7, 8)
    m0, m1 = rr == yy, rr == yy + 1
    for d in range(0, 24, 2):
        r0, r1 = (jnp.concatenate([jnp.broadcast_to(kb[b][d + k:d + k + 1, :], (8, 256)) for k in range(2)], axis=0)
                  for b in range(2))
        L[8 * d:8 * d + 16, :] = jnp.where(m0, r0, jnp.where(m1, r1, F32(0))).astype(jnp.bfloat16)

    def store_pair(p, m, t, x0, x1):
        for j in range(4):
            x = jnp.concatenate([x0[8 * j:8 * j + 8], x1[8 * j:8 * j + 8]], axis=0)
            h = x.astype(jnp.bfloat16)
            UH[p, m, t, j] = h
            g = 2.0 * x - h.astype(F32)
            G[0, p, m, t, 8 * j:8 * j + 8, :] = g[0:8]
            G[1, p, m, t, 8 * j:8 * j + 8, :] = g[8:16]
            if j > 0:
                HR[p, t, 8 * j - 8 + 2 * m:8 * j - 7 + 2 * m, :] = x0[8 * j:8 * j + 1]
                HR[p, t, 8 * j - 7 + 2 * m:8 * j - 6 + 2 * m, :] = x1[8 * j:8 * j + 1]

    def shifted(p, m, t, zx):
        s1 = pltpu.roll(U[p, m, 1], 127, 1)
        if t == 1:
            return jnp.where(lane32 == 127, zx, s1)
        return jnp.where(lane32 == 127, s1, pltpu.roll(U[p, m, 0], 127, 1))

    def prep(p, t, z_row=None, first=0):
        for m in range(3):
            zx = None if t == 0 else pltpu.roll(z_row, 127 - (3 * p + m - first), 1)
            store_pair(p, m, t, U[p, m, t], shifted(p, m, t, zx))

    Gf = G.reshape(2 * (nx + 1) * 3 * 2 * 40, 128)
    HRf = HR.reshape((nx + 1) * 2 * 32, 128)

    def halo_rows(first, count, zx_row, planes):
        lanes = lax.broadcasted_iota(jnp.int32, (count, 128), 1)
        rows = lax.broadcasted_iota(jnp.int32, (count, 128), 0)
        nxt = jnp.sum(jnp.where(lanes == rows, jnp.broadcast_to(zx_row, (count, 128)), 0.0), axis=1, keepdims=True)
        u0, u1 = YH[0, first:first + count, :], YH[1, first:first + count, :]
        s0, s1 = pltpu.roll(u0, 127, 1), pltpu.roll(u1, 127, 1)
        v0 = jnp.where(lanes == 127, s1, s0)
        v1 = jnp.where(lanes == 127, jnp.broadcast_to(nxt, (count, 128)), s1)
        for c, pair in enumerate(((u0, u1), (v0, v1))):
            for t in range(2):
                HY[c, t, first:first + count, :] = pair[t]
                GY[c, t, first:first + count, :] = 2.0 * pair[t] - rounded(pair[t])
        for c in range(2):
            for t in range(2):
                n = 3 * planes
                at = ((c * (nx + 1) + first // 3) * 6 + t) * 40 + 32
                Gf[pl.ds(at, n, stride=80), :] = GY[c, t, first:first + n, :]
                for m in range(3):
                    at = ((first // 3) * 2 + t) * 32 + 24 + 2 * m + c
                    if planes == 1:
                        HRf[at:at + 1, :] = HY[c, t, first + m:first + m + 1, :]
                    else:
                        HRf[pl.ds(at, planes, stride=64), :] = HY[c, t, pl.ds(first + m, planes, stride=3), :]

    def pairs(todo, acc):
        comp, vol = acc
        for pair in todo:
            cols = []
            for i, j, t in pair:
                tiles = [UH[i + a, m, t, j] for a in range(2) for m in range(3)]
                tiles.append(jnp.concatenate(
                    [HR[i, t, 8 * j:8 * j + 8, :], HR[i + 1, t, 8 * j:8 * j + 8, :]], axis=0).astype(jnp.bfloat16))
                cols.append(jnp.concatenate(tiles, axis=0))
            rhs = jnp.concatenate(cols, axis=1)
            rhs = jnp.concatenate([rhs, rhs], axis=0)
            prod = jnp.dot(L[:, 0:224], rhs, preferred_element_type=F32)
            for side, (i, j, t) in enumerate(pair):
                r0 = 8 * j
                e = None
                for d in range(24):
                    m, a, b, c = d // 8, (d // 4) % 2, (d // 2) % 2, d % 2
                    term = prod[8 * d:8 * d + 8, 128 * side:128 * side + 128] * G[c, i + a, m, t, pl.ds(r0 + b, 8), :]
                    e = term if e is None else e + term
                rho = R[i, t, r0:r0 + 8, :]
                r2 = rho * rho
                comp = comp + (VOID + (r2 * rho) * (1.0 - VOID)) * e
                vol = vol + rho
                W[i, t, r0:r0 + 8, :] = (r2 * e) * (INV[t, r0:r0 + 8, :] * taps_sum(gx * nx + i, px * nx))
        return comp, vol

    def half_region(t, z_row, acc):
        for p in range(3):
            prep(p, t, z_row)
        for i in range(0, nx - 2, 2):
            for p in (i + 3, i + 4):
                if p < nx:
                    prep(p, t, z_row)
            acc = pairs([((i, 0, t), (i, 1, t)), ((i + 1, 0, t), (i + 1, 1, t)), ((i, 2, t), (i + 1, 2, t))], acc)
        return acc

    for c in loads[6:8]:
        c.wait()
    with jax.named_scope("c_main0"):
        acc = half_region(0, None, (zero8, zero8))
    wait("w_z", (has_zu, z_copy.wait_recv))
    with jax.named_scope("c_main1"):
        acc = half_region(1, ZX[0, 0:32, :], acc)
        i = nx - 2
        acc = pairs([((i, 0, 0), (i, 1, 0)), ((i, 0, 1), (i, 1, 1)), ((i, 2, 0), (i, 2, 1))], acc)
    wait("w_yz", (both_u, yz_copy.wait_recv))
    wait("w_y", (has_yu, y_copy.wait_recv))
    when(at_corner & has_yu, xy_corner.start)
    when(at_corner & has_zu, xz_corner.start)
    when(at_corner & both_u, xyz_corner.start)
    with jax.named_scope("c_halo"):
        halo_rows(0, nq, ZX[0, 32:33, :], nx)
    with jax.named_scope("c_main2"):
        acc = lax.fori_loop(0, nx - 1, lambda i, a: pairs([((i, 3, 0), (i, 3, 1))], a), acc, unroll=UNROLL_LAST)

    def relay():
        pl.semaphore_wait(go.at[GO_R], 1)
        when(has_yu, xy_to_relay.wait_recv, xy_relay.start)
        when(has_zu, xz_to_relay.wait_recv, xz_relay.start)
        when(both_u, xyz_to_relay.wait_recv, xyz_relay.start)
        xm_to_relay.wait_recv()
        xm_relay.start()

    wait("w_xm", (not_last, xm_copy.wait_recv))
    wait("w_xe", (not_last & has_yu, xy_copy.wait_recv), (not_last & has_zu, xz_copy.wait_recv),
         (not_last & both_u, xyz_copy.wait_recv))
    with jax.named_scope("c_last"):
        prep(nx, 0)
        prep(nx, 1, ZX[1, 0:32, :], 3 * nx)
        halo_rows(nq, 8, ZX[1, 32:33, :], 1)
        i = nx - 1
        comp, vol = pairs([((i, j, 0), (i, j, 1)) for j in range(4)], acc)

    row_of = zc * py + gy

    def row_copy(buf, me, sems, place):
        return pltpu.make_async_remote_copy(
            src_ref=buf.at[me], dst_ref=buf.at[me], send_sem=sems[0], recv_sem=sems[1],
            device_id=dev(*place), device_id_type=MESH)

    def wait_rows(buf, count, sem):
        part = buf.at[pl.ds(0, count)]
        pltpu.make_async_copy(part, part, sem).wait()

    def add_up(rows):
        while len(rows) > 1:
            rows = [a + b for a, b in zip(rows[::2], rows[1::2])] + ([rows[-1]] if len(rows) % 2 else [])
        return rows[0]

    def x_copy(place):
        return row_copy(A1, groups[0][1], (ar_send.at[0], ar_recv.at[0]), place)

    def y_copy_of(place):
        return row_copy(A2, row_of, (ar_send.at[1], ar_recv.at[1]), place)

    def down_copy(z, y):
        return row_copy(A2, row_of, (down_send.at[z], down_recv.at[zc]), (xh * half + z, y, gz))

    def up_copy(z):
        return row_copy(A3, zc, (up_send.at[z], up_recv.at[zc]), (xh * half + z, gy, gz))

    def when_any(number, slot):
        when(number > 0, lambda: pl.semaphore_wait(go.at[slot], number))

    key_y = groups[1][0]

    lane1 = lax.broadcasted_iota(jnp.int32, (1, 128), 1)
    comp_all = jnp.sum(jnp.sum(comp, axis=0, keepdims=True), axis=1, keepdims=True)
    vol_all = jnp.sum(jnp.sum(vol, axis=0, keepdims=True), axis=1, keepdims=True)
    A1[groups[0][1]] = jnp.where(lane1 == 0, jnp.broadcast_to(comp_all, (1, 128)), jnp.broadcast_to(vol_all, (1, 128)))
    wait("w_relay", (first_x, relay))
    with jax.named_scope("w_go0"):
        when_any(npz - 1 - groups[0][0], 0)
    for _, place in members_x():
        x_copy(place).start()
    when(zc > 0, lambda: signal_go(GO_U, gx - 1, gy, gz))

    for t in range(2):
        zr = lax.broadcasted_iota(jnp.int32, (256, 128), 0)
        zl = lax.broadcasted_iota(jnp.int32, (256, 128), 1) + 128 * t
        T[:, 128 * t:128 * t + 128] = jnp.maximum(3 - jnp.abs(zr - zl), 0).astype(F32).astype(jnp.bfloat16)

    with jax.named_scope("c_packw"):
        lo, hi = zero32, zero32
        for p in range(nx):
            w0, w1 = W[p, 0], W[p, 1]
            for k in range(2):
                lo = jnp.where(lane32 == 2 * p + k, jnp.broadcast_to(w0[:, k:k + 1], (32, 128)), lo)
                hi = jnp.where(lane32 == 2 * p + k, jnp.broadcast_to(w1[:, 126 + k:127 + k], (32, 128)), hi)
        even = (lane32 & 1) == 0
        CL[...] = jnp.where(even, lo, lo + 2.0 * pltpu.roll(lo, 1, 1))
        CR[...] = jnp.where(even, hi + 2.0 * pltpu.roll(hi, 127, 1), hi)
    zl_copy = remote(CL, CLr, S_ZL, gx, gy, gz - 1)
    zr_copy = remote(CR, CRr, S_ZR, gx, gy, gz + 1)
    when(has_zl, zl_copy.start)
    when(has_zu, zr_copy.start)

    def filter_z(g, carry):
        w = jnp.concatenate([jnp.concatenate([W[4 * g + k, 0], W[4 * g + k, 1]], axis=1) for k in range(4)], axis=0)
        w_hi = w.astype(jnp.bfloat16)
        w_lo = (w - w_hi.astype(F32)).astype(jnp.bfloat16)
        z = jnp.dot(w_hi, T[...], preferred_element_type=F32) + jnp.dot(w_lo, T[...], preferred_element_type=F32)
        for k in range(4):
            for t in range(2):
                Z[4 * g + k, t, 8:40, :] = z[32 * k:32 * k + 32, 128 * t:128 * t + 128]
        return carry

    with jax.named_scope("c_fz"):
        lax.fori_loop(0, nx // 4, filter_z, 0, unroll=True)

    with jax.named_scope("w_go1"):
        when_any(py - 1 - key_y, 1)
    for other, place in members_y():
        when(other > key_y, lambda: signal_go(GO_T, *place))
    send_go(2)
    wait("w_wz", (has_zu, zl_copy.wait_recv), (has_zl, zr_copy.wait_recv))
    with jax.named_scope("c_fixz"):
        left, right = CRr[...], CLr[...]
        for p in range(nx):
            Z[p, 0, 8:40, :] += jnp.where(lane32 < 2, pltpu.roll(left, (128 - 2 * p) % 128, 1), 0.0)
            Z[p, 1, 8:40, :] += jnp.where(lane32 >= 126, pltpu.roll(right, 126 - 2 * p, 1), 0.0)

    Zf = Z.reshape(nx * 2 * 48, 128)
    for t in range(2):
        for r in range(2):
            YS2[0, t, r * nx:(r + 1) * nx, :] = Zf[pl.ds(48 * t + 8 + r, nx, stride=96), :]
            YS2[1, t, r * nx:(r + 1) * nx, :] = Zf[pl.ds(48 * t + 38 + r, nx, stride=96), :]
    yd_copy = remote(YS2.at[0], YR.at[1], S_YD, gx, gy - 1, gz)
    yu_copy = remote(YS2.at[1], YR.at[0], S_YU, gx, gy + 1, gz)
    when(has_yl, yd_copy.start)
    when(has_yu, lambda: pl.semaphore_wait(go.at[GO_V], 1), yu_copy.start)

    def second_stage():
        with jax.named_scope("w_ar0"):
            wait_rows(A1, npz - 1, ar_recv.at[0])
        A2[row_of] = add_up([A1[k] for k in range(npz)])
        with jax.named_scope("w_got"):
            when_any(key_y, GO_T)
        for z in range(half - 1):
            @pl.when(z < zc)
            def _():
                for dy in range(py):
                    down_copy(z, (gy + hy + dy) % py).start()
        for _, place in members_y():
            y_copy_of(place).start()

    layers_first = lower1 & (gy == 0)
    when(jnp.logical_not(layers_first), second_stage)

    wait("w_wy", (has_yu, yd_copy.wait_recv), (has_yl, yu_copy.wait_recv))
    for t in range(2):
        for r in range(2):
            Zf[pl.ds(48 * t + 6 + r, nx, stride=96), :] = YR[0, t, r * nx:(r + 1) * nx, :]
            Zf[pl.ds(48 * t + 40 + r, nx, stride=96), :] = YR[1, t, r * nx:(r + 1) * nx, :]

    def filter_y(p, carry):
        for t in range(2):
            z = [Z[p, t, 6 + d:38 + d, :] for d in range(5)]
            F[p + 2, t] = 3.0 * z[2] + 2.0 * (z[1] + z[3]) + (z[0] + z[4])
        return carry

    with jax.named_scope("c_fy"):
        lax.fori_loop(0, nx, filter_y, 0, unroll=2)

    xd_copy = remote(F.at[pl.ds(2, 2)], F.at[pl.ds(nx + 2, 2)], S_XD, gx - 1, gy, gz)
    xd_to_relay = remote(F.at[pl.ds(2, 2)], RF, S_RF, 0, gy, gz)
    xd_relay = remote(RF, F.at[pl.ds(nx + 2, 2)], S_XD, half - 1, gy, gz)
    xu_copy = remote(F.at[pl.ds(nx, 2)], F.at[pl.ds(0, 2)], S_XU, gx + 1, gy, gz)
    when(plain_down, xd_copy.start)
    when(upper0, xd_to_relay.start)
    when(zc < half - 1, lambda: pl.semaphore_wait(go.at[GO_U], 1))
    when(not_last, xu_copy.start)
    when(layers_first, second_stage)

    def filter_x(p, carry):
        for t in range(2):
            f = [F[p + d, t] for d in range(5)]
            out[p, :, 128 * t:128 * t + 128] = 3.0 * f[2] + 2.0 * (f[1] + f[3]) + (f[0] + f[4])
        return carry

    wait("w_frelay", (first_x, xd_to_relay.wait_recv, xd_relay.start))
    with jax.named_scope("c_fx"):
        lax.fori_loop(2, nx - 2, filter_x, 0, unroll=2)
    with jax.named_scope("w_ar1"):
        wait_rows(A2, py - 1, ar_recv.at[1])
    A3[zc] = add_up([A2[zc * py + k] for k in range(py)])
    with jax.named_scope("w_go2"):
        when_any(half - 1 - zc, 2)
    for z in range(1, half):
        when(z > zc, up_copy(z).start)

    wait("w_fd", (not_last, xd_copy.wait_recv))
    for p in (nx - 2, nx - 1):
        filter_x(p, 0)
    wait("w_fu", (not_first, xu_copy.wait_recv))
    for p in (0, 1):
        filter_x(p, 0)

    with jax.named_scope("w_sends"):
        when(has_yl, y_copy.wait_send, yd_copy.wait_send)
        when(has_zl, z_copy.wait_send, zl_copy.wait_send)
        when(has_yl & has_zl, yz_copy.wait_send)
        when(has_zu, zr_copy.wait_send)
        when(has_yu, yu_copy.wait_send)
        when(plain_down, xm_copy.wait_send, xd_copy.wait_send)
        when(plain_down & has_yl, xy_copy.wait_send)
        when(plain_down & has_zl, xz_copy.wait_send)
        when(plain_down & both_l, xyz_copy.wait_send)
        when(upper0, xm_to_relay.wait_send, xd_to_relay.wait_send)
        when(upper0 & has_yl & no(skip_y), xy_to_relay.wait_send)
        when(upper0 & has_zl & no(skip_z), xz_to_relay.wait_send)
        when(upper0 & both_l & no(skip_yz), xyz_to_relay.wait_send)
        when(at_corner & has_yu, xy_corner.wait_send)
        when(at_corner & has_zu, xz_corner.wait_send)
        when(at_corner & both_u, xyz_corner.wait_send)
        when(first_x, xm_relay.wait_send, xd_relay.wait_send)
        when(first_x & has_yu, xy_relay.wait_send)
        when(first_x & has_zu, xz_relay.wait_send)
        when(first_x & both_u, xyz_relay.wait_send)
        when(not_last, xu_copy.wait_send)
        wait_rows(A1, npz - 1, ar_send.at[0])
        wait_rows(A2, py - 1, ar_send.at[1])
        for z in range(half):
            when(z < zc, lambda: wait_rows(A2, py, down_send.at[z]))
            when(z > zc, lambda: wait_rows(A3, 1, up_send.at[z]))

    def add_upper(z, c):
        wait_rows(A2, py, down_recv.at[z])
        A3[z] = add_up([A2[z * py + k] for k in range(py)])
        return c

    def add_lower(z, c):
        wait_rows(A3, 1, up_recv.at[z])
        return c

    with jax.named_scope("w_ar2"):
        lax.fori_loop(0, zc, add_lower, 0)
        lax.fori_loop(zc + 1, half, add_upper, 0)
    total = add_up([A3[z] for z in range(half)])
    count = F32(px * nx) * F32(py * ny) * F32(pz * 256)
    sums[...] = jnp.broadcast_to(total / count, (8, 128))


def finish(out_ref, sums_ref, filtered, comp, vol, c_ref, v_ref, sem):
    copies = [pltpu.make_async_copy(out_ref, filtered, sem.at[0])]
    copies[0].start()
    c_ref[...] = sums_ref[0:1, 0:1]
    v_ref[...] = sums_ref[0:1, 1:2]
    for k, (src, dst) in enumerate(((c_ref, comp), (v_ref, vol))):
        copies.append(pltpu.make_async_copy(src, dst, sem.at[1 + k]))
        copies[-1].start()
    for c in copies:
        c.wait()


def on_device(displacement, density, stiffness):
    px, py, pz = lax.axis_size("gx"), lax.axis_size("gy"), lax.axis_size("gz")
    nx, ny, nz = density.shape
    nq = 3 * nx
    vm = lambda *shape: pltpu.VMEM(shape, F32)
    out, sums = pl.pallas_call(
        functools.partial(kernel, nx, ny, px, py, pz),
        out_shape=(jax.ShapeDtypeStruct((nx, ny, nz), F32), jax.ShapeDtypeStruct((8, 128), F32)),
        in_specs=[pl.BlockSpec(memory_space=pltpu.HBM)] * 3,
        out_specs=(pl.BlockSpec(memory_space=pltpu.VMEM), pl.BlockSpec(memory_space=pltpu.VMEM)),
        scratch_shapes=[
            vm(nx + 1, 3, 2, 32, 128),
            pltpu.VMEM((nx + 1, 3, 2, 4, 16, 128), jnp.bfloat16),
            vm(2, nx + 1, 3, 2, 40, 128),
            vm(nx + 1, 2, 32, 128),
            vm(nx, 2, 32, 128),
            vm(nx, 2, 32, 128),
            vm(nx, 2, 48, 128),
            vm(nx + 4, 2, 32, 128),
            pltpu.VMEM((256, 256), jnp.bfloat16),
            pltpu.VMEM((192, 256), jnp.bfloat16),
            vm(24, 24),
            vm(2, 32, 128),
            vm(2, nq, 128),
            vm(2, nq + 8, 128),
            vm(2, 2, nq + 8, 128),
            vm(2, 2, nq + 8, 128),
            vm(32, 128),
            vm(2, 40, 128),
            vm(3, 2, 32, 128),
            vm(2, 8, 128),
            vm(40, 128),
            vm(32, 128), vm(32, 128), vm(32, 128), vm(32, 128),
            vm(2, 2, 2 * nx, 128),
            vm(2, 2, 2 * nx, 128),
            vm(2, 2, 32, 128),
            vm(2 * pz, 1, 128), vm(py * px // 2, 1, 128), vm(px // 2, 1, 128),
            pltpu.SemaphoreType.DMA((9,)),
            pltpu.SemaphoreType.DMA((N_SEM,)),
            pltpu.SemaphoreType.DMA((N_SEM,)),
            pltpu.SemaphoreType.DMA((2,)),
            pltpu.SemaphoreType.DMA((2,)),
            pltpu.SemaphoreType.DMA((px // 2,)),
            pltpu.SemaphoreType.DMA((px // 2,)),
            pltpu.SemaphoreType.DMA((px // 2,)),
            pltpu.SemaphoreType.DMA((px // 2,)),
            pltpu.SemaphoreType.REGULAR((7,)),
        ],
        compiler_params=pltpu.CompilerParams(collective_id=0, has_side_effects=True, vmem_limit_bytes=56_000_000),
    )(displacement, density, pltpu.with_memory_space_constraint(stiffness, pltpu.HBM))
    vmem = pl.BlockSpec(memory_space=pltpu.VMEM)
    out, comp, vol = pl.pallas_call(
        finish,
        out_shape=(jax.ShapeDtypeStruct((nx, ny, nz), F32), jax.ShapeDtypeStruct((1, 1), F32), jax.ShapeDtypeStruct((1, 1), F32)),
        in_specs=[vmem, vmem],
        out_specs=(pl.BlockSpec(memory_space=pltpu.HBM),) * 3,
        scratch_shapes=[pltpu.VMEM((1, 1), F32), pltpu.VMEM((1, 1), F32), pltpu.SemaphoreType.DMA((3,))],
        compiler_params=pltpu.CompilerParams(vmem_limit_bytes=4 << 20),
    )(out, sums)
    return out, comp.reshape(()), vol.reshape(())


def solution(mesh):
    return jax.shard_map(
        on_device,
        mesh=mesh,
        in_specs=(P(None, "gx", "gy", "gz"), P("gx", "gy", "gz"), P()),
        out_specs=(P("gx", "gy", "gz"), P(), P()),
        check_vma=False,
    )
```

```python
import functools

import jax
import jax.numpy as jnp
from jax import lax
from jax.experimental import pallas as pl
from jax.experimental.pallas import tpu as pltpu
from jax.sharding import PartitionSpec as P

VOID = 0.001
MESH = pl.DeviceIdType.MESH
F32 = jnp.float32

S_Y, S_Z, S_YZ, S_XM, S_XY, S_XZ, S_RM, S_RY, S_RZ = range(9)
S_ZL, S_ZR, S_YD, S_YU, S_XD, S_XU, S_RF = range(9, 16)
S_XYZ, S_RYZ = 16, 17
S_HALF = 15
N_SEM = 22
GO_U, GO_R, GO_T, GO_V = 3, 4, 5, 6
UNROLL_LAST = 15


def rounded(v):
    return v.astype(jnp.bfloat16).astype(F32)


def taps_sum(position, extent):
    low = jnp.minimum(position, extent - 1 - position)
    return jnp.where(low == 0, F32(1 / 6), jnp.where(low == 1, F32(1 / 8), F32(1 / 9)))


def kernel(nx, ny, px, py, pz,
           disp, dens, stiff,
           out, sums,
           U, UH, G, HR, R, W, Z, F, T, L, KV, INV,
           YS, YH, HY, GY, ZS, ZX, RU, RY, RZ,
           CL, CR, CLr, CRr, YS2, YR, RF, A1, A2, A3,
           load_sem, send_sem, recv_sem, ar_send, ar_recv, down_send, down_recv, up_send, up_recv, go):
    gx, gy, gz = lax.axis_index("gx"), lax.axis_index("gy"), lax.axis_index("gz")
    half = px // 2
    xh, zc = gx // half, gx % half
    lane32 = lax.broadcasted_iota(jnp.int32, (32, 128), 1)
    nq = 3 * nx
    npz = 2 * pz

    def dev(x, y, z):
        return {"gx": x, "gy": y, "gz": z}

    def remote(src, dst, slot, x, y, z):
        return pltpu.make_async_remote_copy(
            src_ref=src, dst_ref=dst, send_sem=send_sem.at[slot], recv_sem=recv_sem.at[slot],
            device_id=dev(x, y, z), device_id_type=MESH)

    def when(cond, *actions):
        @pl.when(cond)
        def _():
            for act in actions:
                act()

    def wait(name, *pairs):
        with jax.named_scope(name):
            for cond, *actions in pairs:
                when(cond, *actions)

    loads = []
    for t in range(2):
        for m in range(3):
            loads.append(pltpu.make_async_copy(
                disp.at[m, :, :, pl.ds(128 * t, 128)], U.at[pl.ds(0, nx), m, t], load_sem.at[3 * t + m]))
    for t in range(2):
        loads.append(pltpu.make_async_copy(dens.at[:, :, pl.ds(128 * t, 128)], R.at[:, t], load_sem.at[6 + t]))
    k_load = pltpu.make_async_copy(stiff, KV, load_sem.at[8])
    for c in loads[:6] + [k_load]:
        c.start()

    has_yl, has_yu = gy > 0, gy < py - 1
    has_zl, has_zu = gz > 0, gz < pz - 1
    last_x, first_x, upper0, lower1 = gx == px - 1, gx == 0, gx == half, gx == half - 1
    not_last, not_first = gx < px - 1, gx > 0
    plain_down = not_first & (gx != half)

    bar = pltpu.get_barrier_semaphore()

    def signal(x, y, z):
        pl.semaphore_signal(bar, inc=1, device_id=dev(x, y, z), device_id_type=MESH)

    def signal_go(slot, x, y, z):
        pl.semaphore_signal(go.at[slot], inc=1, device_id=dev(x, y, z), device_id_type=MESH)

    def as_int(c):
        return c.astype(jnp.int32)

    nxc, hx, hy = pz, pz // 2, py // 2
    at_origin = lambda c: jnp.where(c, 1, 0)
    ox = at_origin((gy == 0) & (zc == 0))
    oy = at_origin((gx == 0) & (gz == 0))

    def x_rank(x):
        return jnp.where(x < hx, x, nxc - 1 + hx - x)

    def y_rank(y):
        return jnp.where(y < hy, y, py - 1 + hy - y)

    my_x, core = xh * hx + gz // 2, gz % 2

    def members_x():
        for dx in (4, 3, 5, 2, 6, 1, 7, 0) if nxc == 8 else range(nxc):
            for dc in range(2):
                if dx or dc:
                    x, c = (my_x + dx) % nxc, (core + dc) % 2
                    yield key_of_x(x, c), ((x // hx) * half + zc, gy, 2 * (x % hx) + c)

    def members_y():
        for d in (4, 3, 5, 2, 6, 1, 7) if py == 8 else range(1, py):
            y = (gy + d) % py
            yield key_of_y(y), (gx, y, gz)

    def members_z():
        for d in range(1, half):
            z = (zc + d) % half
            yield z, (xh * half + z, gy, gz)

    def key_of_x(x, c):
        return (2 * x_rank(x) + 1 - c + npz - 2 * ox) % npz

    def key_of_y(y):
        return (y_rank(y) + py - oy) % py

    groups = ((key_of_x(my_x, core), 2 * my_x + core, npz, members_x),
              (key_of_y(gy), gy, py, members_y),
              (zc, zc, half, members_z))

    def send_go(slot):
        key, _, _, members = groups[slot]
        for other, place in members():
            when(other < key, lambda: signal_go(slot, *place))

    when(has_zu, lambda: signal(gx, gy, gz + 1))
    when(has_zl, lambda: signal(gx, gy, gz - 1))
    when(has_yu, lambda: signal(gx, gy + 1, gz))
    when(has_yu & has_zu, lambda: signal(gx, gy + 1, gz + 1))
    when(upper0, lambda: signal(half - 1, gy, gz))

    def edges(x, cond):
        when(cond & has_yu, lambda: signal(x, gy + 1, gz))
        when(cond & has_zu, lambda: signal(x, gy, gz + 1))
        when(cond & has_yu & has_zu, lambda: signal(x, gy + 1, gz + 1))

    when(first_x, lambda: signal(half, gy, gz))
    edges(gx + 1, not_last & (gx != half - 1))
    edges(half, first_x & ((gy > 0) | (gz > 0)))
    skip_y, skip_z, skip_yz = (upper0 & (gy == y) & (gz == z) for y, z in ((1, 0), (0, 1), (1, 1)))
    at_corner = upper0 & (gy == 0) & (gz == 0)
    when((gx == half + half // 2 - 1) & (gy < 2) & (gz < 2) & (gy + gz > 0), lambda: signal(half, gy, gz))
    def of_x(k):
        r = (k + 2 * ox) % npz
        x = x_rank(r // 2)
        return (x // hx) * half + zc, gy, 2 * (x % hx) + 1 - r % 2

    def of_y(k):
        return gx, y_rank((k + oy) % py), gz

    def of_z(k):
        return xh * half + k, gy, gz

    for (key, _, count, _), place in zip((groups[1], groups[2], groups[0]), (of_y, of_z, of_x)):
        def tell(k, c, place=place):
            signal(*place(k))
            return c

        lax.fori_loop(key + 1, count, tell, 0)
    n_wait = as_int(has_zu) + as_int(has_zl) + as_int(has_yl) + as_int(has_yl & has_zl) + as_int(lower1 | upper0)
    n_wait = n_wait + groups[0][0] + groups[1][0] + groups[2][0]
    n_wait = n_wait + jnp.where(first_x, 0, as_int(has_yl) + as_int(has_zl) + as_int(has_yl & has_zl))

    for c in loads[6:]:
        c.start()
    with jax.named_scope("w_bar0"):
        when(lower1, lambda: pl.semaphore_wait(bar, n_wait), lambda: signal_go(GO_R, 0, gy, gz))

    zero32 = jnp.zeros((32, 128), F32)
    with jax.named_scope("w_load0"):
        for c in loads[:3]:
            c.wait()
    Uf = U.reshape((nx + 1) * 3 * 2 * 32, 128)
    with jax.named_scope("c_packz"):
        acc = zero32
        for q in range(nq):
            acc = jnp.where(lane32 == q, jnp.broadcast_to(U[q // 3, q % 3, 0, :, 0:1], (32, 128)), acc)
        ZS[...] = acc
        YS[0] = Uf[pl.ds(0, nq, stride=64), :]
    with jax.named_scope("w_load1"):
        for c in loads[3:6]:
            c.wait()
    YS[1] = Uf[pl.ds(32, nq, stride=64), :]

    with jax.named_scope("w_bar"):
        when(jnp.logical_not(lower1), lambda: pl.semaphore_wait(bar, n_wait))

    y_copy = remote(YS, YH.at[:, pl.ds(0, nq), :], S_Y, gx, gy - 1, gz)
    z_copy = remote(ZS, ZX.at[0, pl.ds(0, 32), :], S_Z, gx, gy, gz - 1)
    yz_copy = remote(ZS.at[pl.ds(0, 8), :], ZX.at[0, pl.ds(32, 8), :], S_YZ, gx, gy - 1, gz - 1)
    xm_copy, xm_to_relay, xm_relay = ([f(t) for t in range(2)] for f in (
        lambda t: remote(U.at[0, :, t], U.at[nx, :, t], S_XM + t * S_HALF, gx - 1, gy, gz),
        lambda t: remote(U.at[0, :, t], RU.at[:, t], S_RM + t * S_HALF, 0, gy, gz),
        lambda t: remote(RU.at[:, t], U.at[nx, :, t], S_XM + t * S_HALF, half - 1, gy, gz)))
    xy_copy = remote(YS.at[:, pl.ds(0, 8), :], YH.at[:, pl.ds(nq, 8), :], S_XY, gx - 1, gy - 1, gz)
    xy_to_relay = remote(YS.at[:, pl.ds(0, 8), :], RY, S_RY, 0, gy - 1, gz)
    xy_relay = remote(RY, YH.at[:, pl.ds(nq, 8), :], S_XY, half - 1, gy, gz)
    xz_copy = remote(ZS, ZX.at[1, pl.ds(0, 32), :], S_XZ, gx - 1, gy, gz - 1)
    xz_to_relay = remote(ZS, RZ.at[pl.ds(0, 32), :], S_RZ, 0, gy, gz - 1)
    xz_relay = remote(RZ.at[pl.ds(0, 32), :], ZX.at[1, pl.ds(0, 32), :], S_XZ, half - 1, gy, gz)
    xyz_copy = remote(ZS.at[pl.ds(0, 8), :], ZX.at[1, pl.ds(32, 8), :], S_XYZ, gx - 1, gy - 1, gz - 1)
    xyz_to_relay = remote(ZS.at[pl.ds(0, 8), :], RZ.at[pl.ds(32, 8), :], S_RYZ, 0, gy - 1, gz - 1)
    xyz_relay = remote(RZ.at[pl.ds(32, 8), :], ZX.at[1, pl.ds(32, 8), :], S_XYZ, half - 1, gy, gz)
    both_l, both_u = has_yl & has_zl, has_yu & has_zu

    when(has_zl, z_copy.start)
    when(has_yl & has_zl, yz_copy.start)
    when(has_yl, y_copy.start)
    when(plain_down, xm_copy[1].start, xm_copy[0].start)
    when(upper0, xm_to_relay[1].start, xm_to_relay[0].start)
    when(plain_down & has_yl, xy_copy.start)
    when(plain_down & has_zl, xz_copy.start)
    when(plain_down & both_l, xyz_copy.start)
    no = jnp.logical_not
    when(upper0 & has_yl & no(skip_y), xy_to_relay.start)
    when(upper0 & has_zl & no(skip_z), xz_to_relay.start)
    when(upper0 & both_l & no(skip_yz), xyz_to_relay.start)
    xy_corner = remote(YH.at[:, pl.ds(0, 8), :], RY, S_RY, 0, gy, gz)
    xz_corner = remote(ZX.at[0, pl.ds(0, 32), :], RZ.at[pl.ds(0, 32), :], S_RZ, 0, gy, gz)
    xyz_corner = remote(ZX.at[0, pl.ds(32, 8), :], RZ.at[pl.ds(32, 8), :], S_RYZ, 0, gy, gz)

    when(has_yl, lambda: signal_go(GO_V, gx, gy - 1, gz))
    send_go(0)
    send_go(1)

    zero8 = jnp.zeros((8, 128), F32)

    @pl.when(last_x)
    def _():
        for m in range(3):
            for t in range(2):
                U[nx, m, t] = zero32
        for t in range(2):
            YH[t, nq:nq + 8, :] = zero8
            F[nx + 2, t] = zero32
            F[nx + 3, t] = zero32
        ZX[1] = jnp.zeros((40, 128), F32)

    @pl.when(first_x)
    def _():
        for t in range(2):
            F[0, t] = zero32
            F[1, t] = zero32

    @pl.when(gy == py - 1)
    def _():
        for t in range(2):
            YH[t] = jnp.zeros((nq + 8, 128), F32)
            YR[1, t] = jnp.zeros((2 * nx, 128), F32)

    @pl.when(gy == 0)
    def _():
        for t in range(2):
            YR[0, t] = jnp.zeros((2 * nx, 128), F32)

    @pl.when(gz == pz - 1)
    def _():
        ZX[0, 0:32, :] = zero32
        ZX[1, 0:32, :] = zero32
        CLr[...] = zero32

    @pl.when((gz == pz - 1) | (gy == py - 1))
    def _():
        ZX[0, 32:40, :] = zero8
        ZX[1, 32:40, :] = zero8

    @pl.when(gz == 0)
    def _():
        CRr[...] = zero32

    for t in range(2):
        yv = lax.broadcasted_iota(jnp.int32, (32, 128), 0) + gy * ny
        zv = lane32 + 128 * t + gz * 256
        INV[t] = (F32(-3.0 * (1.0 - VOID)) * taps_sum(yv, py * ny)) * taps_sum(zv, pz * 256)
    HR[...] = jnp.zeros(HR.shape, F32)

    k_load.wait()
    kv = KV[...]
    k_hi = rounded(kv)
    k_lo = kv - k_hi
    dr = lax.broadcasted_iota(jnp.int32, (24, 256), 0)
    cc = lax.broadcasted_iota(jnp.int32, (24, 256), 1)
    second = cc >= 112
    cl = jnp.where(second, cc - 112, cc)
    inside = cc < 224
    tau = cl >> 3
    in_main = cl < 96
    a_m = as_int(tau >= 6)
    a_ = jnp.where(in_main, a_m, (cl - 96) >> 3)
    mc_ = jnp.where(in_main, tau - 6 * a_m, cl & 7)
    ok = inside & (mc_ < 6)
    d0 = 8 * (mc_ >> 1) + 4 * a_ + (mc_ & 1)
    kb = []
    for b in range(2):
        pick = ok & (dr == d0 + 2 * b)
        b_hi = jnp.where(pick & jnp.logical_not(second), F32(1), F32(0))
        b_lo = jnp.where(pick & second, F32(1), F32(0))
        kb.append(jnp.dot(k_hi, b_hi, preferred_element_type=F32) + jnp.dot(k_lo, b_lo, preferred_element_type=F32))
    cy = lax.broadcasted_iota(jnp.int32, (16, 256), 1)
    yy = lax.broadcasted_iota(jnp.int32, (16, 256), 0) & 7
    cy = jnp.where(cy >= 112, cy - 112, cy)
    rr = jnp.where(cy < 96, cy & 7, 8)
    m0, m1 = rr == yy, rr == yy + 1
    for d in range(0, 24, 2):
        r0, r1 = (jnp.concatenate([jnp.broadcast_to(kb[b][d + k:d + k + 1, :], (8, 256)) for k in range(2)], axis=0)
                  for b in range(2))
        L[8 * d:8 * d + 16, :] = jnp.where(m0, r0, jnp.where(m1, r1, F32(0))).astype(jnp.bfloat16)

    def store_pair(p, m, t, x0, x1):
        for j in range(4):
            x = jnp.concatenate([x0[8 * j:8 * j + 8], x1[8 * j:8 * j + 8]], axis=0)
            h = x.astype(jnp.bfloat16)
            UH[p, m, t, j] = h
            g = 2.0 * x - h.astype(F32)
            G[0, p, m, t, 8 * j:8 * j + 8, :] = g[0:8]
            G[1, p, m, t, 8 * j:8 * j + 8, :] = g[8:16]
            if j > 0:
                HR[p, t, 8 * j - 8 + 2 * m:8 * j - 7 + 2 * m, :] = x0[8 * j:8 * j + 1]
                HR[p, t, 8 * j - 7 + 2 * m:8 * j - 6 + 2 * m, :] = x1[8 * j:8 * j + 1]

    def shifted(p, m, t, zx):
        s1 = pltpu.roll(U[p, m, 1], 127, 1)
        if t == 1:
            return jnp.where(lane32 == 127, zx, s1)
        return jnp.where(lane32 == 127, s1, pltpu.roll(U[p, m, 0], 127, 1))

    def prep(p, t, z_row=None, first=0):
        for m in range(3):
            zx = None if t == 0 else pltpu.roll(z_row, 127 - (3 * p + m - first), 1)
            store_pair(p, m, t, U[p, m, t], shifted(p, m, t, zx))

    Gf = G.reshape(2 * (nx + 1) * 3 * 2 * 40, 128)
    HRf = HR.reshape((nx + 1) * 2 * 32, 128)

    def halo_rows(first, count, zx_row, planes):
        lanes = lax.broadcasted_iota(jnp.int32, (count, 128), 1)
        rows = lax.broadcasted_iota(jnp.int32, (count, 128), 0)
        nxt = jnp.sum(jnp.where(lanes == rows, jnp.broadcast_to(zx_row, (count, 128)), 0.0), axis=1, keepdims=True)
        u0, u1 = YH[0, first:first + count, :], YH[1, first:first + count, :]
        s0, s1 = pltpu.roll(u0, 127, 1), pltpu.roll(u1, 127, 1)
        v0 = jnp.where(lanes == 127, s1, s0)
        v1 = jnp.where(lanes == 127, jnp.broadcast_to(nxt, (count, 128)), s1)
        for c, pair in enumerate(((u0, u1), (v0, v1))):
            for t in range(2):
                HY[c, t, first:first + count, :] = pair[t]
                GY[c, t, first:first + count, :] = 2.0 * pair[t] - rounded(pair[t])
        for c in range(2):
            for t in range(2):
                n = 3 * planes
                at = ((c * (nx + 1) + first // 3) * 6 + t) * 40 + 32
                Gf[pl.ds(at, n, stride=80), :] = GY[c, t, first:first + n, :]
                for m in range(3):
                    at = ((first // 3) * 2 + t) * 32 + 24 + 2 * m + c
                    if planes == 1:
                        HRf[at:at + 1, :] = HY[c, t, first + m:first + m + 1, :]
                    else:
                        HRf[pl.ds(at, planes, stride=64), :] = HY[c, t, pl.ds(first + m, planes, stride=3), :]

    def pairs(todo, acc):
        comp, vol = acc
        for pair in todo:
            cols = []
            for i, j, t in pair:
                tiles = [UH[i + a, m, t, j] for a in range(2) for m in range(3)]
                tiles.append(jnp.concatenate(
                    [HR[i, t, 8 * j:8 * j + 8, :], HR[i + 1, t, 8 * j:8 * j + 8, :]], axis=0).astype(jnp.bfloat16))
                cols.append(jnp.concatenate(tiles, axis=0))
            rhs = jnp.concatenate(cols, axis=1)
            rhs = jnp.concatenate([rhs, rhs], axis=0)
            prod = jnp.dot(L[:, 0:224], rhs, preferred_element_type=F32)
            for side, (i, j, t) in enumerate(pair):
                r0 = 8 * j
                e = None
                for d in range(24):
                    m, a, b, c = d // 8, (d // 4) % 2, (d // 2) % 2, d % 2
                    term = prod[8 * d:8 * d + 8, 128 * side:128 * side + 128] * G[c, i + a, m, t, pl.ds(r0 + b, 8), :]
                    e = term if e is None else e + term
                rho = R[i, t, r0:r0 + 8, :]
                r2 = rho * rho
                comp = comp + (VOID + (r2 * rho) * (1.0 - VOID)) * e
                vol = vol + rho
                W[i, t, r0:r0 + 8, :] = (r2 * e) * (INV[t, r0:r0 + 8, :] * taps_sum(gx * nx + i, px * nx))
        return comp, vol

    def half_region(t, z_row, acc):
        for p in range(3):
            prep(p, t, z_row)
        for i in range(0, nx - 2, 2):
            for p in (i + 3, i + 4):
                if p < nx:
                    prep(p, t, z_row)
            acc = pairs([((i, 0, t), (i, 1, t)), ((i + 1, 0, t), (i + 1, 1, t)), ((i, 2, t), (i + 1, 2, t))], acc)
        return acc

    for c in loads[6:8]:
        c.wait()
    with jax.named_scope("c_main0"):
        acc = half_region(0, None, (zero8, zero8))
    wait("w_z", (has_zu, z_copy.wait_recv))
    with jax.named_scope("c_main1"):
        acc = half_region(1, ZX[0, 0:32, :], acc)
        i = nx - 2
        acc = pairs([((i, 0, 0), (i, 1, 0)), ((i, 0, 1), (i, 1, 1)), ((i, 2, 0), (i, 2, 1))], acc)
    wait("w_yz", (both_u, yz_copy.wait_recv))
    wait("w_y", (has_yu, y_copy.wait_recv))
    when(at_corner & has_yu, xy_corner.start)
    when(at_corner & has_zu, xz_corner.start)
    when(at_corner & both_u, xyz_corner.start)
    with jax.named_scope("c_halo"):
        halo_rows(0, nq, ZX[0, 32:33, :], nx)
    with jax.named_scope("c_main2"):
        acc = lax.fori_loop(0, nx - 1, lambda i, a: pairs([((i, 3, 0), (i, 3, 1))], a), acc, unroll=UNROLL_LAST)

    def relay():
        pl.semaphore_wait(go.at[GO_R], 1)
        when(has_yu, xy_to_relay.wait_recv, xy_relay.start)
        when(has_zu, xz_to_relay.wait_recv, xz_relay.start)
        when(both_u, xyz_to_relay.wait_recv, xyz_relay.start)
        for t in (1, 0):
            xm_to_relay[t].wait_recv()
            xm_relay[t].start()

    wait("w_xe", (not_last & has_yu, xy_copy.wait_recv), (not_last & has_zu, xz_copy.wait_recv),
         (not_last & both_u, xyz_copy.wait_recv))
    i = nx - 1
    halo_rows(nq, 8, ZX[1, 32:33, :], 1)
    for t in (1, 0):
        wait("w_xm", (not_last, xm_copy[t].wait_recv))
        with jax.named_scope("c_last"):
            prep(nx, t, ZX[1, 0:32, :], 3 * nx)
            acc = pairs([((i, 0, t), (i, 1, t)), ((i, 2, t), (i, 3, t))], acc)
    comp, vol = acc

    row_of = zc * py + gy

    def row_copy(buf, me, sems, place):
        return pltpu.make_async_remote_copy(
            src_ref=buf.at[me], dst_ref=buf.at[me], send_sem=sems[0], recv_sem=sems[1],
            device_id=dev(*place), device_id_type=MESH)

    def wait_rows(buf, count, sem):
        part = buf.at[pl.ds(0, count)]
        pltpu.make_async_copy(part, part, sem).wait()

    def add_up(rows):
        while len(rows) > 1:
            rows = [a + b for a, b in zip(rows[::2], rows[1::2])] + ([rows[-1]] if len(rows) % 2 else [])
        return rows[0]

    def x_copy(place):
        return row_copy(A1, groups[0][1], (ar_send.at[0], ar_recv.at[0]), place)

    def y_copy_of(place):
        return row_copy(A2, row_of, (ar_send.at[1], ar_recv.at[1]), place)

    def down_copy(z, y):
        return row_copy(A2, row_of, (down_send.at[z], down_recv.at[zc]), (xh * half + z, y, gz))

    def up_copy(z):
        return row_copy(A3, zc, (up_send.at[z], up_recv.at[zc]), (xh * half + z, gy, gz))

    def when_any(number, slot):
        when(number > 0, lambda: pl.semaphore_wait(go.at[slot], number))

    key_y = groups[1][0]

    lane1 = lax.broadcasted_iota(jnp.int32, (1, 128), 1)
    comp_all = jnp.sum(jnp.sum(comp, axis=0, keepdims=True), axis=1, keepdims=True)
    vol_all = jnp.sum(jnp.sum(vol, axis=0, keepdims=True), axis=1, keepdims=True)
    A1[groups[0][1]] = jnp.where(lane1 == 0, jnp.broadcast_to(comp_all, (1, 128)), jnp.broadcast_to(vol_all, (1, 128)))
    wait("w_relay", (first_x, relay))
    with jax.named_scope("w_go0"):
        when_any(npz - 1 - groups[0][0], 0)
    for _, place in members_x():
        x_copy(place).start()
    when(zc > 0, lambda: signal_go(GO_U, gx - 1, gy, gz))

    for t in range(2):
        zr = lax.broadcasted_iota(jnp.int32, (256, 128), 0)
        zl = lax.broadcasted_iota(jnp.int32, (256, 128), 1) + 128 * t
        T[:, 128 * t:128 * t + 128] = jnp.maximum(3 - jnp.abs(zr - zl), 0).astype(F32).astype(jnp.bfloat16)

    with jax.named_scope("c_packw"):
        lo, hi = zero32, zero32
        for p in range(nx):
            w0, w1 = W[p, 0], W[p, 1]
            for k in range(2):
                lo = jnp.where(lane32 == 2 * p + k, jnp.broadcast_to(w0[:, k:k + 1], (32, 128)), lo)
                hi = jnp.where(lane32 == 2 * p + k, jnp.broadcast_to(w1[:, 126 + k:127 + k], (32, 128)), hi)
        even = (lane32 & 1) == 0
        CL[...] = jnp.where(even, lo, lo + 2.0 * pltpu.roll(lo, 1, 1))
        CR[...] = jnp.where(even, hi + 2.0 * pltpu.roll(hi, 127, 1), hi)
    zl_copy = remote(CL, CLr, S_ZL, gx, gy, gz - 1)
    zr_copy = remote(CR, CRr, S_ZR, gx, gy, gz + 1)
    when(has_zl, zl_copy.start)
    when(has_zu, zr_copy.start)

    def filter_z(g, carry):
        w = jnp.concatenate([jnp.concatenate([W[4 * g + k, 0], W[4 * g + k, 1]], axis=1) for k in range(4)], axis=0)
        w_hi = w.astype(jnp.bfloat16)
        w_lo = (w - w_hi.astype(F32)).astype(jnp.bfloat16)
        z = jnp.dot(w_hi, T[...], preferred_element_type=F32) + jnp.dot(w_lo, T[...], preferred_element_type=F32)
        for k in range(4):
            for t in range(2):
                Z[4 * g + k, t, 8:40, :] = z[32 * k:32 * k + 32, 128 * t:128 * t + 128]
        return carry

    with jax.named_scope("c_fz"):
        lax.fori_loop(0, nx // 4, filter_z, 0, unroll=True)

    with jax.named_scope("w_go1"):
        when_any(py - 1 - key_y, 1)
    for other, place in members_y():
        when(other > key_y, lambda: signal_go(GO_T, *place))
    send_go(2)
    wait("w_wz", (has_zu, zl_copy.wait_recv), (has_zl, zr_copy.wait_recv))
    with jax.named_scope("c_fixz"):
        left, right = CRr[...], CLr[...]
        for p in range(nx):
            Z[p, 0, 8:40, :] += jnp.where(lane32 < 2, pltpu.roll(left, (128 - 2 * p) % 128, 1), 0.0)
            Z[p, 1, 8:40, :] += jnp.where(lane32 >= 126, pltpu.roll(right, 126 - 2 * p, 1), 0.0)

    Zf = Z.reshape(nx * 2 * 48, 128)
    for t in range(2):
        for r in range(2):
            YS2[0, t, r * nx:(r + 1) * nx, :] = Zf[pl.ds(48 * t + 8 + r, nx, stride=96), :]
            YS2[1, t, r * nx:(r + 1) * nx, :] = Zf[pl.ds(48 * t + 38 + r, nx, stride=96), :]
    yd_copy = remote(YS2.at[0], YR.at[1], S_YD, gx, gy - 1, gz)
    yu_copy = remote(YS2.at[1], YR.at[0], S_YU, gx, gy + 1, gz)
    when(has_yl, yd_copy.start)
    when(has_yu, lambda: pl.semaphore_wait(go.at[GO_V], 1), yu_copy.start)

    def second_stage():
        with jax.named_scope("w_ar0"):
            wait_rows(A1, npz - 1, ar_recv.at[0])
        A2[row_of] = add_up([A1[k] for k in range(npz)])
        with jax.named_scope("w_got"):
            when_any(key_y, GO_T)
        for z in range(half - 1):
            @pl.when(z < zc)
            def _():
                for dy in range(py):
                    down_copy(z, (gy + hy + dy) % py).start()
        for _, place in members_y():
            y_copy_of(place).start()

    layers_first = lower1 & (gy == 0)
    when(jnp.logical_not(layers_first), second_stage)

    wait("w_wy", (has_yu, yd_copy.wait_recv), (has_yl, yu_copy.wait_recv))
    for t in range(2):
        for r in range(2):
            Zf[pl.ds(48 * t + 6 + r, nx, stride=96), :] = YR[0, t, r * nx:(r + 1) * nx, :]
            Zf[pl.ds(48 * t + 40 + r, nx, stride=96), :] = YR[1, t, r * nx:(r + 1) * nx, :]

    def filter_y(p, carry):
        for t in range(2):
            z = [Z[p, t, 6 + d:38 + d, :] for d in range(5)]
            F[p + 2, t] = 3.0 * z[2] + 2.0 * (z[1] + z[3]) + (z[0] + z[4])
        return carry

    with jax.named_scope("c_fy"):
        lax.fori_loop(0, nx, filter_y, 0, unroll=2)

    xd_copy = remote(F.at[pl.ds(2, 2)], F.at[pl.ds(nx + 2, 2)], S_XD, gx - 1, gy, gz)
    xd_to_relay = remote(F.at[pl.ds(2, 2)], RF, S_RF, 0, gy, gz)
    xd_relay = remote(RF, F.at[pl.ds(nx + 2, 2)], S_XD, half - 1, gy, gz)
    xu_copy = remote(F.at[pl.ds(nx, 2)], F.at[pl.ds(0, 2)], S_XU, gx + 1, gy, gz)
    when(plain_down, xd_copy.start)
    when(upper0, xd_to_relay.start)
    when(zc < half - 1, lambda: pl.semaphore_wait(go.at[GO_U], 1))
    when(not_last, xu_copy.start)
    when(layers_first, second_stage)

    def filter_x(p, carry):
        for t in range(2):
            f = [F[p + d, t] for d in range(5)]
            out[p, :, 128 * t:128 * t + 128] = 3.0 * f[2] + 2.0 * (f[1] + f[3]) + (f[0] + f[4])
        return carry

    wait("w_frelay", (first_x, xd_to_relay.wait_recv, xd_relay.start))
    with jax.named_scope("c_fx"):
        lax.fori_loop(2, nx - 2, filter_x, 0, unroll=2)
    with jax.named_scope("w_ar1"):
        wait_rows(A2, py - 1, ar_recv.at[1])
    A3[zc] = add_up([A2[zc * py + k] for k in range(py)])
    with jax.named_scope("w_go2"):
        when_any(half - 1 - zc, 2)
    for z in range(1, half):
        when(z > zc, up_copy(z).start)

    wait("w_fd", (not_last, xd_copy.wait_recv))
    for p in (nx - 2, nx - 1):
        filter_x(p, 0)
    wait("w_fu", (not_first, xu_copy.wait_recv))
    for p in (0, 1):
        filter_x(p, 0)

    with jax.named_scope("w_sends"):
        when(has_yl, y_copy.wait_send, yd_copy.wait_send)
        when(has_zl, z_copy.wait_send, zl_copy.wait_send)
        when(has_yl & has_zl, yz_copy.wait_send)
        when(has_zu, zr_copy.wait_send)
        when(has_yu, yu_copy.wait_send)
        when(plain_down, xm_copy[0].wait_send, xm_copy[1].wait_send, xd_copy.wait_send)
        when(plain_down & has_yl, xy_copy.wait_send)
        when(plain_down & has_zl, xz_copy.wait_send)
        when(plain_down & both_l, xyz_copy.wait_send)
        when(upper0, xm_to_relay[0].wait_send, xm_to_relay[1].wait_send, xd_to_relay.wait_send)
        when(upper0 & has_yl & no(skip_y), xy_to_relay.wait_send)
        when(upper0 & has_zl & no(skip_z), xz_to_relay.wait_send)
        when(upper0 & both_l & no(skip_yz), xyz_to_relay.wait_send)
        when(at_corner & has_yu, xy_corner.wait_send)
        when(at_corner & has_zu, xz_corner.wait_send)
        when(at_corner & both_u, xyz_corner.wait_send)
        when(first_x, xm_relay[0].wait_send, xm_relay[1].wait_send, xd_relay.wait_send)
        when(first_x & has_yu, xy_relay.wait_send)
        when(first_x & has_zu, xz_relay.wait_send)
        when(first_x & both_u, xyz_relay.wait_send)
        when(not_last, xu_copy.wait_send)
        wait_rows(A1, npz - 1, ar_send.at[0])
        wait_rows(A2, py - 1, ar_send.at[1])
        for z in range(half):
            when(z < zc, lambda: wait_rows(A2, py, down_send.at[z]))
            when(z > zc, lambda: wait_rows(A3, 1, up_send.at[z]))

    def add_upper(z, c):
        wait_rows(A2, py, down_recv.at[z])
        A3[z] = add_up([A2[z * py + k] for k in range(py)])
        return c

    def add_lower(z, c):
        wait_rows(A3, 1, up_recv.at[z])
        return c

    with jax.named_scope("w_ar2"):
        lax.fori_loop(0, zc, add_lower, 0)
        lax.fori_loop(zc + 1, half, add_upper, 0)
    total = add_up([A3[z] for z in range(half)])
    count = F32(px * nx) * F32(py * ny) * F32(pz * 256)
    sums[...] = jnp.broadcast_to(total / count, (8, 128))


def finish(out_ref, sums_ref, filtered, comp, vol, c_ref, v_ref, sem):
    copies = [pltpu.make_async_copy(out_ref, filtered, sem.at[0])]
    copies[0].start()
    c_ref[...] = sums_ref[0:1, 0:1]
    v_ref[...] = sums_ref[0:1, 1:2]
    for k, (src, dst) in enumerate(((c_ref, comp), (v_ref, vol))):
        copies.append(pltpu.make_async_copy(src, dst, sem.at[1 + k]))
        copies[-1].start()
    for c in copies:
        c.wait()


def on_device(displacement, density, stiffness):
    px, py, pz = lax.axis_size("gx"), lax.axis_size("gy"), lax.axis_size("gz")
    nx, ny, nz = density.shape
    nq = 3 * nx
    vm = lambda *shape: pltpu.VMEM(shape, F32)
    out, sums = pl.pallas_call(
        functools.partial(kernel, nx, ny, px, py, pz),
        out_shape=(jax.ShapeDtypeStruct((nx, ny, nz), F32), jax.ShapeDtypeStruct((8, 128), F32)),
        in_specs=[pl.BlockSpec(memory_space=pltpu.HBM)] * 3,
        out_specs=(pl.BlockSpec(memory_space=pltpu.VMEM), pl.BlockSpec(memory_space=pltpu.VMEM)),
        scratch_shapes=[
            vm(nx + 1, 3, 2, 32, 128),
            pltpu.VMEM((nx + 1, 3, 2, 4, 16, 128), jnp.bfloat16),
            vm(2, nx + 1, 3, 2, 40, 128),
            vm(nx + 1, 2, 32, 128),
            vm(nx, 2, 32, 128),
            vm(nx, 2, 32, 128),
            vm(nx, 2, 48, 128),
            vm(nx + 4, 2, 32, 128),
            pltpu.VMEM((256, 256), jnp.bfloat16),
            pltpu.VMEM((192, 256), jnp.bfloat16),
            vm(24, 24),
            vm(2, 32, 128),
            vm(2, nq, 128),
            vm(2, nq + 8, 128),
            vm(2, 2, nq + 8, 128),
            vm(2, 2, nq + 8, 128),
            vm(32, 128),
            vm(2, 40, 128),
            vm(3, 2, 32, 128),
            vm(2, 8, 128),
            vm(40, 128),
            vm(32, 128), vm(32, 128), vm(32, 128), vm(32, 128),
            vm(2, 2, 2 * nx, 128),
            vm(2, 2, 2 * nx, 128),
            vm(2, 2, 32, 128),
            vm(2 * pz, 1, 128), vm(py * px // 2, 1, 128), vm(px // 2, 1, 128),
            pltpu.SemaphoreType.DMA((9,)),
            pltpu.SemaphoreType.DMA((N_SEM,)),
            pltpu.SemaphoreType.DMA((N_SEM,)),
            pltpu.SemaphoreType.DMA((2,)),
            pltpu.SemaphoreType.DMA((2,)),
            pltpu.SemaphoreType.DMA((px // 2,)),
            pltpu.SemaphoreType.DMA((px // 2,)),
            pltpu.SemaphoreType.DMA((px // 2,)),
            pltpu.SemaphoreType.DMA((px // 2,)),
            pltpu.SemaphoreType.REGULAR((7,)),
        ],
        compiler_params=pltpu.CompilerParams(collective_id=0, has_side_effects=True, vmem_limit_bytes=56_000_000),
    )(displacement, density, pltpu.with_memory_space_constraint(stiffness, pltpu.HBM))
    vmem = pl.BlockSpec(memory_space=pltpu.VMEM)
    out, comp, vol = pl.pallas_call(
        finish,
        out_shape=(jax.ShapeDtypeStruct((nx, ny, nz), F32), jax.ShapeDtypeStruct((1, 1), F32), jax.ShapeDtypeStruct((1, 1), F32)),
        in_specs=[vmem, vmem],
        out_specs=(pl.BlockSpec(memory_space=pltpu.HBM),) * 3,
        scratch_shapes=[pltpu.VMEM((1, 1), F32), pltpu.VMEM((1, 1), F32), pltpu.SemaphoreType.DMA((3,))],
        compiler_params=pltpu.CompilerParams(vmem_limit_bytes=4 << 20),
    )(out, sums)
    return out, comp.reshape(()), vol.reshape(())


def solution(mesh):
    return jax.shard_map(
        on_device,
        mesh=mesh,
        in_specs=(P(None, "gx", "gy", "gz"), P("gx", "gy", "gz"), P()),
        out_specs=(P("gx", "gy", "gz"), P(), P()),
        check_vma=False,
    )
```
